32 devices in a mesh: ep: 32 (over z, y, x, core).
Axes of the slice: x: 2, y: 2, z: 4, core: 2. Of those that a mesh axis runs over, the one named last changes fastest.
Arguments:
- hidden: bfloat16 [2, 1024, 3584], P(None, 'ep'), may hold values from -6 to 6
- expert_ids: int32 [2, 1024, 8], P(None, 'ep'), may hold values from 0 to 31, all different within a row; in each aligned block of 32 rows (0 to 31, 32 to 63, ..., all dimensions but the last counted through in order) at most 9 rows name the same one
- gate_scores: float32 [2, 1024, 8], P(None, 'ep'), may hold values from 0.05 to 1
- w_gate: bfloat16 [32, 3584, 1024], P('ep'), may hold values from -0.09375 to 0.09375
- w_up: bfloat16 [32, 3584, 1024], P('ep'), may hold values from -0.09375 to 0.09375
- w_down: bfloat16 [32, 1024, 3584], P('ep'), may hold values from -0.1875 to 0.1875
Outputs:
- mixed: bfloat16 [2, 1024, 3584], P(None, 'ep')
- expert_load: float32 [32], P('ep')
The draws below stay inside these ranges and needn't reach their ends.
Inputs may be any that keep to these rules, and one draw needn't show every extreme that they name: `expert_ids`: among the 32 rows of one device in one micro-batch, no expert is named by more than 9 rows, a bound that some block reaches. Each row names 8 different experts.
All inputs are finite; a program needn't handle non-finite values.
Results may differ from the reference program's by a relative error of at most 0.004.
The reference program's roundings to bfloat16 on the way (of `hid` and `answer`) count: a program that leaves them out, or rounds other values in their place, can miss the bound.
Values may be sent and summed in bfloat16 or wider, within the bound.
A program may use at most 128 MiB of HBM per device.

```python
import math
import jax
import jax.numpy as jnp
import numpy as np
from jax import lax

D = 3584
FF = 1024
TOP = 8
MICRO = 2
TOK_MB = 32
EXPERTS = 32
TOKENS = 1024
CAP = 9
N_EP = 32


def levels(own_key, extent, split, least, largest):
    factor_of = 1.0
    for axis_at, shards_of in split:
        heights = jax.random.uniform(jax.random.fold_in(jax.random.fold_in(own_key, 6), axis_at), (shards_of,), jnp.float32, least / len(split), largest / len(split))
        factor_of = factor_of * jnp.repeat(jnp.exp(heights), extent[axis_at] // shards_of).reshape((-1,) + (1,) * (len(extent) - 1 - axis_at))
    return factor_of


def shared_out(key, own, number, rows, count, top, most, skew):
    order = jax.random.permutation(key, count)
    heavy_load, ordinary = load_shares(count, rows * top, most, skew, True), load_shares(count, rows * top, most, skew, False)
    places = jnp.arange(count)

    def named(lengths, turn):
        used = int((lengths > 0).sum())
        fixed = max(1, used // 4)
        moved = fixed + (places - fixed + turn * (used - fixed)) % max(1, count - fixed)
        return jnp.zeros((count,), jnp.int32).at[order[jnp.where(places < fixed, places, moved)]].set(jnp.asarray(lengths, jnp.int32))

    lengths = jnp.where(number % 4 == 0, named(heavy_load, number // 4), named(ordinary, number - number // 4 - 1))
    mixed = jax.random.permutation(jax.random.fold_in(own, 3), count)
    source_of, receiver = mixed[0:count // 2 * 2:2], mixed[1:count // 2 * 2:2]
    slack = jnp.minimum(lengths[source_of] - 1, most - lengths[receiver]) // 2
    slack = jnp.where((source_of == order[0]) | (receiver == order[0]) | (lengths[receiver] == 0), 0, jnp.maximum(slack, 0))
    moved = jax.random.randint(jax.random.fold_in(own, 4), (count // 2,), 0, 1 << 20) % (slack + 1)
    lengths = lengths.at[source_of].add(-moved).at[receiver].add(moved)
    members = jnp.searchsorted(jnp.cumsum(lengths), jnp.arange(rows * top), side="right").astype(jnp.int32)
    table = members.reshape(top, rows).T
    table = table[jax.random.permutation(jax.random.fold_in(own, 1), rows)]
    turn = jax.random.randint(jax.random.fold_in(own, 2), (rows, 1), 0, top)
    return jnp.take_along_axis(table, (jnp.arange(top)[None, :] + turn) % top, axis=1)


def load_shares(amount, total, limit, lean, full):
    loads = [(1 << 20) // math.isqrt(rank ** lean) + 1 for rank in range(1, amount + 1)]
    largest = limit if full else min(limit, max(-(-total // amount), total * loads[0] // sum(loads)))
    least = 1 if total - largest >= amount - 1 else 0
    holding, rest = [largest] + [least] * (amount - 1), total - largest - least * (amount - 1)
    while rest > 0:
        candidates = [i for i in range(1, amount) if holding[i] < largest] or [i for i in range(1, amount) if holding[i] < limit]
        mass, left = sum([loads[i] for i in candidates]), rest
        for i in candidates:
            extra = min(limit - holding[i], max(1, left * loads[i] // mass), rest)
            holding[i] = holding[i] + extra
            rest = rest - extra
    return np.array(holding)


def noise(stream_key, shape, deviation, bound, shards=(), kind=jnp.bfloat16):
    values = jax.random.normal(stream_key, shape, jnp.float32) * deviation
    if len(shards) > 0:
        values = levels(stream_key, shape, shards, -0.22, 0.18) * values
    return jnp.clip(values, min=-bound, max=bound).astype(kind)


def setup_inputs(seed: int = 0) -> dict:
    arg_keys = jax.random.split(jax.random.key(seed), 7)
    hidden = noise(arg_keys[0], (MICRO, TOKENS, D), 1.0, 6.0, ((1, 32),))
    expert_ids_keys = jax.random.split(jax.random.fold_in(arg_keys[1], 1), MICRO * TOKENS // TOK_MB)
    expert_ids_turns = jax.random.permutation(jax.random.fold_in(arg_keys[1], 3), MICRO * TOKENS // TOK_MB)
    expert_ids = jax.vmap(lambda own, number: shared_out(jax.random.fold_in(arg_keys[1], 2), own, number, TOK_MB, EXPERTS, TOP, CAP, 2))(expert_ids_keys, expert_ids_turns).reshape((MICRO, TOKENS, TOP))
    gate_scores = jnp.clip(jnp.exp(math.log(1.0) - 2.9957323 * jax.random.uniform(arg_keys[2], (MICRO, TOKENS, TOP), jnp.float32) ** levels(arg_keys[2], (MICRO, TOKENS, TOP), ((1, 32),), -0.2, 0.2)), 0.05, 1.0)
    w_gate = noise(arg_keys[3], (EXPERTS, D, FF), D ** -0.5, 0.09375, ((0, 32),))
    w_up = noise(arg_keys[4], (EXPERTS, D, FF), D ** -0.5, 0.09375, ((0, 32),))
    w_down = noise(arg_keys[5], (EXPERTS, FF, D), FF ** -0.5, 0.1875, ((0, 32),))
    return dict(hidden=hidden, expert_ids=expert_ids, gate_scores=gate_scores, w_gate=w_gate, w_up=w_up, w_down=w_down)


route_scale = 2.5


def reference(hidden, expert_ids, gate_scores, w_gate, w_up, w_down):
    weights = route_scale * gate_scores / jnp.sum(gate_scores, axis=-1, keepdims=True)
    grouped = expert_ids.reshape(MICRO, N_EP, TOK_MB * TOP)
    one_hot = (grouped[..., None] == jnp.arange(EXPERTS, dtype=jnp.int32)).astype(jnp.int32)
    earlier = jnp.cumsum(one_hot, axis=2) - one_hot
    slot_index = jnp.sum(earlier * one_hot, axis=-1).astype(jnp.int32)
    batch_axis = jnp.arange(MICRO, dtype=jnp.int32)[:, None, None]
    source_axis = jnp.arange(N_EP, dtype=jnp.int32)[None, :, None]
    owner = (jnp.arange(TOK_MB * TOP, dtype=jnp.int32) // TOP)[None, None, :]
    token_row = (owner + source_axis * TOK_MB + batch_axis * TOKENS).astype(jnp.int32)
    table = jnp.full((MICRO, EXPERTS, N_EP, CAP), MICRO * TOKENS, jnp.int32)
    table = table.at[batch_axis, grouped, source_axis, slot_index].set(token_row)
    shares = jnp.zeros((MICRO, EXPERTS, N_EP, CAP), jnp.float32)
    shares = shares.at[batch_axis, grouped, source_axis, slot_index].set(weights.reshape(MICRO, N_EP, TOK_MB * TOP))
    padded = jnp.concatenate([hidden.reshape(MICRO * TOKENS, D), jnp.zeros((1, D), jnp.bfloat16)], axis=0)

    def expert_step(total, expert):
        rows_index = table[:, expert].reshape(-1)
        gathered = padded[rows_index]
        gate = jnp.dot(gathered, w_gate[expert], preferred_element_type=jnp.float32)
        upper = jnp.dot(gathered, w_up[expert], preferred_element_type=jnp.float32)
        hid = (jax.nn.silu(gate) * upper).astype(jnp.bfloat16)
        answer = jnp.dot(hid, w_down[expert], preferred_element_type=jnp.float32).astype(jnp.bfloat16)
        scaled = shares[:, expert].reshape(-1)[:, None] * answer.astype(jnp.float32)
        return total.at[rows_index].add(scaled), None

    start = jnp.zeros((MICRO * TOKENS + 1, D), jnp.float32)
    total, unused = lax.scan(expert_step, start, jnp.arange(EXPERTS, dtype=jnp.int32))
    mixed = total[: MICRO * TOKENS].reshape(MICRO, TOKENS, D).astype(jnp.bfloat16)
    sums = jnp.zeros((EXPERTS,), jnp.float32).at[expert_ids.reshape(-1)].add(weights.reshape(-1))
    expert_load = sums * (EXPERTS / (route_scale * MICRO * TOKENS))
    return mixed, expert_load
```

```python
import functools

import jax
import jax.numpy as jnp
from jax import lax
from jax.experimental import pallas as pl
from jax.experimental.pallas import tpu as pltpu
from jax.sharding import PartitionSpec as P

route_scale = 2.5
PLANE = 8
SLOTS = 3
LAG = 2
MESH = pl.DeviceIdType.MESH


def tri(size, block):
    row = lax.broadcasted_iota(jnp.int32, (size, size), 0)
    col = lax.broadcasted_iota(jnp.int32, (size, size), 1)
    earlier = (row < col) & (lax.div(row, block) == lax.div(col, block))
    return jnp.where(earlier, 1.0, 0.0).astype(jnp.bfloat16)


def layer_kernel(
    planes,
    capacity,
    tok_mb,
    load_scale,
    x_ref,
    ids_ref,
    scores_ref,
    gate_ref,
    up_ref,
    down_ref,
    out_ref,
    load_ref,
    notes,
    column,
    picks,
    shares,
    packed,
    rows,
    loads,
    loads_in,
    w_gate,
    w_up,
    w_down,
    acc_gate,
    acc_up,
    hid,
    inbox,
    sums_in,
    gate_sem,
    up_sem,
    down_sem,
    n_send,
    n_recv,
    x_send,
    x_recv,
    l_send,
    l_recv,
    d_send,
    d_recv,
    a_send,
    a_recv,
    s_send,
    s_recv,
):
    me = lax.axis_index("ep")
    p = me // PLANE
    q = me % PLANE
    chunks, _, tokens, width = column.shape
    chosen = ids_ref.shape[1]
    spots = packed.shape[2]
    depth = planes * tokens

    def cut(c):
        return pl.ds(pl.multiple_of(c * width, width), width)

    def load_in(c):
        slot = c % SLOTS
        return (
            pltpu.make_async_copy(gate_ref.at[cut(c), :], w_gate.at[slot], gate_sem.at[slot]),
            pltpu.make_async_copy(up_ref.at[cut(c), :], w_up.at[slot], up_sem.at[slot]),
        )

    def load_down(c):
        return pltpu.make_async_copy(down_ref.at[:, cut(c)], w_down.at[c], down_sem.at[c])

    for c in range(SLOTS):
        for copy in load_in(c):
            copy.start()

    barrier = pltpu.get_barrier_semaphore()
    for i in range(1, PLANE):
        other = p * PLANE + (q + i) % PLANE
        pl.semaphore_signal(barrier, inc=1, device_id=(other,), device_id_type=MESH)
    for i in range(1, planes):
        other = ((p + i) % planes) * PLANE + q
        pl.semaphore_signal(barrier, inc=1, device_id=(other,), device_id_type=MESH)

    notes[p] = jnp.zeros(notes.shape[1:], jnp.float32)
    scores = scores_ref[...]
    notes[p, 0, :, :chosen] = ids_ref[...].astype(jnp.float32)
    notes[p, 1, :, :chosen] = route_scale * scores / jnp.sum(scores, axis=1, keepdims=True)

    pl.semaphore_wait(barrier, PLANE + planes - 2)

    def along(i):
        return (p + i) % planes

    def beside(i):
        return (q + i) % PLANE

    def up_down(src, dst, send, recv, i):
        return pltpu.make_async_remote_copy(
            src_ref=src,
            dst_ref=dst,
            send_sem=send,
            recv_sem=recv,
            device_id=(along(i) * PLANE + q,),
            device_id_type=MESH,
        )

    def across(src, dst, send, recv, i):
        return pltpu.make_async_remote_copy(
            src_ref=src,
            dst_ref=dst,
            send_sem=send,
            recv_sem=recv,
            device_id=(p * PLANE + beside(i),),
            device_id_type=MESH,
        )

    def notes_copy(i, at):
        return up_down(notes.at[p], notes.at[at], n_send.at[i], n_recv.at[at], i)

    def x_copy(c, i, at):
        return up_down(x_ref.at[:, cut(c)], column.at[c, at], x_send.at[c, i], x_recv.at[c, at], i)

    def loads_copy(i, at):
        return across(loads.at[beside(i)], loads_in.at[at], l_send.at[i], l_recv.at[at], i)

    def rows_copy(c, i, at):
        return across(packed.at[c, beside(i)], rows.at[c, at], d_send.at[c, i], d_recv.at[c, at], i)

    def answer_copy(c, i, at):
        return across(packed.at[c, beside(i)], inbox.at[c, at], a_send.at[c, i], a_recv.at[c, at], i)

    def sum_copy(c, i, at):
        return up_down(column.at[c, along(i)], sums_in.at[c, at], s_send.at[c, i], s_recv.at[c, at], i)

    for i in range(1, planes):
        notes_copy(i, p).start()

    def send_x(c, carry):
        for i in range(1, planes):
            x_copy(c, i, p).start()
        column[c, p] = x_ref[:, cut(c)]
        return carry

    lax.fori_loop(0, chunks, send_x, 0)

    for c in range(chunks):
        load_down(c).start()

    for i in range(1, planes):
        notes_copy(i, along(i)).wait_recv()

    ids = notes[:, 0].reshape(depth, 128).T[:chosen]
    weights = notes[:, 1].reshape(depth, 128).T[:chosen]
    expert = (p * PLANE + lax.broadcasted_iota(jnp.int32, (PLANE, depth), 0)).astype(jnp.float32)
    named = jnp.zeros((PLANE, depth), jnp.float32)
    share = jnp.zeros((PLANE, depth), jnp.float32)
    for k in range(chosen):
        same = jnp.broadcast_to(ids[k : k + 1], (PLANE, depth)) == expert
        named += jnp.where(same, 1.0, 0.0)
        share += jnp.where(same, jnp.broadcast_to(weights[k : k + 1], (PLANE, depth)), 0.0)
    for j in range(PLANE):
        own = jnp.sum(share[j : j + 1], axis=1, keepdims=True)
        loads[j] = jnp.broadcast_to(own, loads.shape[1:])
    for i in range(1, PLANE):
        loads_copy(i, q).start()

    earlier = tri(128, tok_mb)
    rank = jnp.concatenate(
        [
            jnp.dot(
                named[:, at : at + 128].astype(jnp.bfloat16),
                earlier,
                preferred_element_type=jnp.float32,
            )
            for at in range(0, depth, 128)
        ],
        axis=1,
    )
    start = lax.div(lax.broadcasted_iota(jnp.int32, (PLANE, depth), 1), tok_mb) * capacity
    spot = jnp.where(named > 0.5, start.astype(jnp.float32) + rank, -1.0)
    place = lax.broadcasted_iota(jnp.int32, (spots, depth), 0).astype(jnp.float32)
    for j in range(PLANE):
        found = place == jnp.broadcast_to(spot[j : j + 1], (spots, depth))
        picks[j] = jnp.where(found, 1.0, 0.0).astype(jnp.bfloat16)

    def dispatch(c):
        for i in range(1, planes):
            x_copy(c, i, along(i)).wait_recv()
        tokens_here = column[c].reshape(depth, width)
        found = jnp.dot(
            picks[...].reshape(PLANE * spots, depth),
            tokens_here,
            preferred_element_type=jnp.float32,
        )
        packed[c] = found.reshape(packed.shape[1:]).astype(jnp.bfloat16)
        for i in range(1, PLANE):
            rows_copy(c, i, q).start()
        rows[c, q] = packed[c, q]

    def consume(c):
        for copy in load_in(c):
            copy.wait()
        for i in range(1, PLANE):
            rows_copy(c, i, beside(i)).wait_recv()
        slot = c % SLOTS
        got = rows[c].reshape(PLANE * spots, width)
        acc_gate[...] += jnp.dot(got, w_gate[slot], preferred_element_type=jnp.float32)
        acc_up[...] += jnp.dot(got, w_up[slot], preferred_element_type=jnp.float32)

        @pl.when(c + SLOTS < chunks)
        def _():
            for copy in load_in(c + SLOTS):
                copy.start()

    acc_gate[...] = jnp.zeros(acc_gate.shape, jnp.float32)
    acc_up[...] = jnp.zeros(acc_up.shape, jnp.float32)

    def step(c, carry):
        pl.when(c < chunks)(lambda: dispatch(c))
        pl.when(c >= LAG)(lambda: consume(c - LAG))
        return carry

    lax.fori_loop(0, LAG, step, 0)

    both = jnp.concatenate(
        [spot, share, jnp.zeros((128 - 2 * PLANE, depth), jnp.float32)], axis=0
    ).T
    lane = lax.broadcasted_iota(jnp.int32, (depth, 128), 1).astype(jnp.float32)
    for j in range(PLANE):
        found = lane == jnp.broadcast_to(both[:, j : j + 1], (depth, 128))
        held = jnp.broadcast_to(both[:, PLANE + j : PLANE + j + 1], (depth, 128))
        held = jnp.where(found, held, 0.0)
        high = held.astype(jnp.bfloat16)
        shares[j, 0] = high[:, :spots]
        shares[j, 1] = (held - high.astype(jnp.float32)).astype(jnp.bfloat16)[:, :spots]

    lax.fori_loop(LAG, chunks + LAG, step, 0)

    gate = acc_gate[...]
    hid[...] = (gate / (1.0 + jnp.exp(-gate)) * acc_up[...]).astype(jnp.bfloat16)

    def compute(c, carry):
        load_down(c).wait()
        for i in range(1, PLANE):
            rows_copy(c, i, q).wait_send()
        found = jnp.dot(hid[...], w_down[c], preferred_element_type=jnp.float32)
        packed[c] = found.reshape(packed.shape[1:]).astype(jnp.bfloat16)
        for i in range(1, PLANE):
            answer_copy(c, i, q).start()
        inbox[c, q] = packed[c, q]
        return carry

    lax.fori_loop(0, chunks, compute, 0)

    for i in range(1, PLANE):
        loads_copy(i, beside(i)).wait_recv()
    loads_in[q] = loads[q]
    load_ref[...] = (jnp.sum(loads_in[...], axis=0) * load_scale)[:1, :1]

    def combine(c, carry):
        for i in range(1, PLANE):
            answer_copy(c, i, beside(i)).wait_recv()
        total = jnp.zeros((depth, width), jnp.float32)
        for k in range(PLANE):
            for half in range(2):
                total += jnp.dot(shares[k, half], inbox[c, k], preferred_element_type=jnp.float32)
        column[c] = total.reshape(column.shape[1:]).astype(jnp.bfloat16)
        for i in range(1, planes):
            sum_copy(c, i, p).start()
        sums_in[c, p] = column[c, p]
        return carry

    lax.fori_loop(0, chunks, combine, 0)

    def gather_sums(c, carry):
        for i in range(1, planes):
            sum_copy(c, i, along(i)).wait_recv()
        total = sums_in[c, 0].astype(jnp.float32)
        for k in range(1, planes):
            total += sums_in[c, k].astype(jnp.float32)
        out_ref[:, cut(c)] = total.astype(jnp.bfloat16)
        return carry

    lax.fori_loop(0, chunks, gather_sums, 0)

    for i in range(1, planes):
        notes_copy(i, p).wait_send()
    for i in range(1, PLANE):
        loads_copy(i, q).wait_send()

    def finish(c, carry):
        for i in range(1, PLANE):
            answer_copy(c, i, q).wait_send()
        for i in range(1, planes):
            x_copy(c, i, p).wait_send()
            sum_copy(c, i, p).wait_send()
        return carry

    lax.fori_loop(0, chunks, finish, 0)


def layer(x, ids, scores, gate, up, down, devices, tok_mb, capacity, load_scale):
    planes = devices // PLANE
    tokens, model_width = x.shape
    inner = gate.shape[1]
    width = next(w for w in (512, 256, 128) if model_width % w == 0)
    chunks = model_width // width
    spots = planes * (tokens // tok_mb) * capacity
    dma = pltpu.SemaphoreType.DMA
    vmem = pl.BlockSpec(memory_space=pltpu.VMEM)
    hbm = pl.BlockSpec(memory_space=pl.ANY)
    bf16, f32 = jnp.bfloat16, jnp.float32
    return pl.pallas_call(
        functools.partial(layer_kernel, planes, capacity, tok_mb, load_scale),
        out_shape=(
            jax.ShapeDtypeStruct((tokens, model_width), bf16),
            jax.ShapeDtypeStruct((1, 1), f32),
        ),
        in_specs=[vmem, vmem, vmem, hbm, hbm, hbm],
        out_specs=(vmem, vmem),
        scratch_shapes=[
            pltpu.VMEM((planes, 2, tokens, 128), f32),
            pltpu.VMEM((chunks, planes, tokens, width), bf16),
            pltpu.VMEM((PLANE, spots, planes * tokens), bf16),
            pltpu.VMEM((PLANE, 2, planes * tokens, spots), bf16),
            pltpu.VMEM((chunks, PLANE, spots, width), bf16),
            pltpu.VMEM((chunks, PLANE, spots, width), bf16),
            pltpu.VMEM((PLANE, 8, 128), f32),
            pltpu.VMEM((PLANE, 8, 128), f32),
            pltpu.VMEM((SLOTS, width, inner), bf16),
            pltpu.VMEM((SLOTS, width, inner), bf16),
            pltpu.VMEM((chunks, inner, width), bf16),
            pltpu.VMEM((PLANE * spots, inner), f32),
            pltpu.VMEM((PLANE * spots, inner), f32),
            pltpu.VMEM((PLANE * spots, inner), bf16),
            pltpu.VMEM((chunks, PLANE, spots, width), bf16),
            pltpu.VMEM((chunks, planes, tokens, width), bf16),
            dma((SLOTS,)),
            dma((SLOTS,)),
            dma((chunks,)),
            dma((planes,)),
            dma((planes,)),
            dma((chunks, planes)),
            dma((chunks, planes)),
            dma((PLANE,)),
            dma((PLANE,)),
            dma((chunks, PLANE)),
            dma((chunks, PLANE)),
            dma((chunks, PLANE)),
            dma((chunks, PLANE)),
            dma((chunks, planes)),
            dma((chunks, planes)),
        ],
        compiler_params=pltpu.CompilerParams(
            collective_id=0, has_side_effects=True, vmem_limit_bytes=66 * 1000 * 1000
        ),
    )(x, ids, scores, gate, up, down)


def shards(hidden, expert_ids, gate_scores, w_gate, w_up, w_down):
    devices = lax.axis_size("ep")
    micro_count, tok_mb, model_width = hidden.shape
    chosen = expert_ids.shape[2]
    capacity = tok_mb * chosen // devices + 1
    tokens = micro_count * tok_mb
    mixed, expert_load = layer(
        hidden.reshape(tokens, model_width),
        expert_ids.reshape(tokens, chosen),
        gate_scores.reshape(tokens, chosen),
        w_gate[0],
        w_up[0],
        w_down[0],
        devices,
        tok_mb,
        capacity,
        devices / (route_scale * tokens * devices),
    )
    return (mixed.reshape(micro_count, tok_mb, model_width), expert_load.reshape(1))


def solution(mesh):
    placed = (
        P(None, "ep", None),
        P(None, "ep", None),
        P(None, "ep", None),
        P("ep", None, None),
        P("ep", None, None),
        P("ep", None, None),
    )
    return jax.shard_map(
        shards,
        mesh=mesh,
        in_specs=placed,
        out_specs=(P(None, "ep", None), P("ep")),
        check_vma=False,
    )
```

```python
import functools

import jax
import jax.numpy as jnp
from jax import lax
from jax.experimental import pallas as pl
from jax.experimental.pallas import tpu as pltpu
from jax.sharding import PartitionSpec as P

route_scale = 2.5
PLANE = 8
SLOTS = 3
LAG = 3
MESH = pl.DeviceIdType.MESH


def tri(size, block):
    row = lax.broadcasted_iota(jnp.int32, (size, size), 0)
    col = lax.broadcasted_iota(jnp.int32, (size, size), 1)
    earlier = (row < col) & (lax.div(row, block) == lax.div(col, block))
    return jnp.where(earlier, 1.0, 0.0).astype(jnp.bfloat16)


def layer_kernel(
    planes,
    capacity,
    tok_mb,
    load_scale,
    hidden_ref,
    ids_ref,
    scores_ref,
    gate_ref,
    up_ref,
    down_ref,
    out_ref,
    load_ref,
    x_ref,
    notes,
    column,
    picks,
    shares,
    packed,
    rows,
    loads,
    loads_in,
    w_gate,
    w_up,
    w_down,
    acc_gate,
    acc_up,
    hid,
    inbox,
    sums_in,
    hidden_sem,
    gate_sem,
    up_sem,
    down_sem,
    n_send,
    n_recv,
    x_send,
    x_recv,
    l_send,
    l_recv,
    d_send,
    d_recv,
    a_send,
    a_recv,
    s_send,
    s_recv,
):
    me = lax.axis_index("ep")
    p = me // PLANE
    q = me % PLANE
    chunks, _, tokens, width = column.shape
    micro_count, chosen, _ = ids_ref.shape
    spots = packed.shape[2]
    depth = planes * tokens

    def cut(c):
        return pl.ds(pl.multiple_of(c * width, width), width)

    def load_in(c):
        slot = c % SLOTS
        return (
            pltpu.make_async_copy(gate_ref.at[cut(c), :], w_gate.at[slot], gate_sem.at[slot]),
            pltpu.make_async_copy(up_ref.at[cut(c), :], w_up.at[slot], up_sem.at[slot]),
        )

    def load_down(c):
        return pltpu.make_async_copy(down_ref.at[:, cut(c)], w_down.at[c], down_sem.at[c])

    hidden_copy = pltpu.make_async_copy(hidden_ref, x_ref, hidden_sem)
    hidden_copy.start()

    barrier = pltpu.get_barrier_semaphore()
    for i in range(1, PLANE):
        other = p * PLANE + (q + i) % PLANE
        pl.semaphore_signal(barrier, inc=1, device_id=(other,), device_id_type=MESH)
    for i in range(1, planes):
        other = ((p + i) % planes) * PLANE + q
        pl.semaphore_signal(barrier, inc=1, device_id=(other,), device_id_type=MESH)

    for c in range(SLOTS):
        for copy in load_in(c):
            copy.start()

    notes[p] = jnp.zeros(notes.shape[1:], jnp.float32)
    for m in range(micro_count):
        scores = scores_ref[m]
        notes[p, m, 0, :, :tok_mb] = ids_ref[m].astype(jnp.float32)
        notes[p, m, 1, :, :tok_mb] = route_scale * scores / jnp.sum(scores, axis=0, keepdims=True)
    hidden_copy.wait()

    pl.semaphore_wait(barrier, PLANE + planes - 2)

    def along(i):
        return (p + i) % planes

    def beside(i):
        return (q + i) % PLANE

    def up_down(src, dst, send, recv, i):
        return pltpu.make_async_remote_copy(
            src_ref=src,
            dst_ref=dst,
            send_sem=send,
            recv_sem=recv,
            device_id=(along(i) * PLANE + q,),
            device_id_type=MESH,
        )

    def across(src, dst, send, recv, i):
        return pltpu.make_async_remote_copy(
            src_ref=src,
            dst_ref=dst,
            send_sem=send,
            recv_sem=recv,
            device_id=(p * PLANE + beside(i),),
            device_id_type=MESH,
        )

    def notes_copy(i, at):
        return up_down(notes.at[p], notes.at[at], n_send.at[i], n_recv.at[at], i)

    def x_copy(c, i, at):
        return up_down(x_ref.at[:, cut(c)], column.at[c, at], x_send.at[c, i], x_recv.at[c, at], i)

    def loads_copy(i, at):
        return across(loads.at[beside(i)], loads_in.at[at], l_send.at[i], l_recv.at[at], i)

    def rows_copy(c, i, at):
        return across(packed.at[c, beside(i)], rows.at[c, at], d_send.at[c, i], d_recv.at[c, at], i)

    def answer_copy(c, i, at):
        return across(packed.at[c, beside(i)], inbox.at[c, at], a_send.at[c, i], a_recv.at[c, at], i)

    def sum_copy(c, i, at):
        return up_down(column.at[c, along(i)], sums_in.at[c, at], s_send.at[c, i], s_recv.at[c, at], i)

    for i in range(1, planes):
        notes_copy(i, p).start()

    def send_x(c, carry):
        for i in range(1, planes):
            x_copy(c, i, p).start()
        column[c, p] = x_ref[:, cut(c)]
        return carry

    lax.fori_loop(0, chunks, send_x, 0)

    for c in range(chunks):
        load_down(c).start()

    for i in range(1, planes):
        notes_copy(i, along(i)).wait_recv()

    def spread(part):
        pieces = [notes[at, m, part] for at in range(planes) for m in range(micro_count)]
        lanes = []
        for at in range(0, len(pieces), 128 // tok_mb):
            block = pieces[at]
            for k, piece in enumerate(pieces[at + 1 : at + 128 // tok_mb]):
                block += pltpu.roll(piece, (k + 1) * tok_mb, 1)
            lanes.append(block)
        return jnp.concatenate(lanes, axis=1)

    ids, weights = spread(0), spread(1)
    expert = (p * PLANE + lax.broadcasted_iota(jnp.int32, (PLANE, depth), 0)).astype(jnp.float32)
    named = jnp.zeros((PLANE, depth), jnp.float32)
    share = jnp.zeros((PLANE, depth), jnp.float32)
    for k in range(chosen):
        same = jnp.broadcast_to(ids[k : k + 1], (PLANE, depth)) == expert
        named += jnp.where(same, 1.0, 0.0)
        share += jnp.where(same, jnp.broadcast_to(weights[k : k + 1], (PLANE, depth)), 0.0)
    for j in range(PLANE):
        own = jnp.sum(share[j : j + 1], axis=1, keepdims=True)
        loads[j] = jnp.broadcast_to(own, loads.shape[1:])
    for i in range(1, PLANE):
        loads_copy(i, q).start()

    earlier = tri(128, tok_mb)
    rank = jnp.concatenate(
        [
            jnp.dot(
                named[:, at : at + 128].astype(jnp.bfloat16),
                earlier,
                preferred_element_type=jnp.float32,
            )
            for at in range(0, depth, 128)
        ],
        axis=1,
    )
    start = lax.div(lax.broadcasted_iota(jnp.int32, (PLANE, depth), 1), tok_mb) * capacity
    spot = jnp.where(named > 0.5, start.astype(jnp.float32) + rank, -1.0)
    place = lax.broadcasted_iota(jnp.int32, (spots, depth), 0).astype(jnp.float32)
    for j in range(PLANE):
        found = place == jnp.broadcast_to(spot[j : j + 1], (spots, depth))
        picks[j] = jnp.where(found, 1.0, 0.0).astype(jnp.bfloat16)

    def dispatch(c):
        for i in range(1, planes):
            x_copy(c, i, along(i)).wait_recv()
        tokens_here = column[c].reshape(depth, width)
        found = jnp.dot(
            picks[...].reshape(PLANE * spots, depth),
            tokens_here,
            preferred_element_type=jnp.float32,
        )
        packed[c] = found.reshape(packed.shape[1:]).astype(jnp.bfloat16)
        for i in range(1, PLANE):
            rows_copy(c, i, q).start()
        rows[c, q] = packed[c, q]

    def consume(c):
        for copy in load_in(c):
            copy.wait()
        for i in range(1, PLANE):
            rows_copy(c, i, beside(i)).wait_recv()
        slot = c % SLOTS
        got = rows[c].reshape(PLANE * spots, width)
        acc_gate[...] += jnp.dot(got, w_gate[slot], preferred_element_type=jnp.float32)
        acc_up[...] += jnp.dot(got, w_up[slot], preferred_element_type=jnp.float32)

        @pl.when(c + SLOTS < chunks)
        def _():
            for copy in load_in(c + SLOTS):
                copy.start()

    acc_gate[...] = jnp.zeros(acc_gate.shape, jnp.float32)
    acc_up[...] = jnp.zeros(acc_up.shape, jnp.float32)

    def step(c, carry):
        pl.when(c < chunks)(lambda: dispatch(c))
        pl.when(c >= LAG)(lambda: consume(c - LAG))
        return carry

    lax.fori_loop(0, LAG, step, 0)

    both = jnp.concatenate(
        [spot, share, jnp.zeros((128 - 2 * PLANE, depth), jnp.float32)], axis=0
    ).T
    lane = lax.broadcasted_iota(jnp.int32, (depth, 128), 1).astype(jnp.float32)
    for j in range(PLANE):
        found = lane == jnp.broadcast_to(both[:, j : j + 1], (depth, 128))
        held = jnp.broadcast_to(both[:, PLANE + j : PLANE + j + 1], (depth, 128))
        held = jnp.where(found, held, 0.0)
        high = held.astype(jnp.bfloat16)
        shares[j, 0] = high[:, :spots]
        shares[j, 1] = (held - high.astype(jnp.float32)).astype(jnp.bfloat16)[:, :spots]

    lax.fori_loop(LAG, chunks + LAG, step, 0)

    gate = acc_gate[...]
    hid[...] = (gate / (1.0 + jnp.exp(-gate)) * acc_up[...]).astype(jnp.bfloat16)

    def compute(c, carry):
        load_down(c).wait()
        for i in range(1, PLANE):
            rows_copy(c, i, q).wait_send()
        found = jnp.dot(hid[...], w_down[c], preferred_element_type=jnp.float32)
        packed[c] = found.reshape(packed.shape[1:]).astype(jnp.bfloat16)
        for i in range(1, PLANE):
            answer_copy(c, i, q).start()
        inbox[c, q] = packed[c, q]
        return carry

    lax.fori_loop(0, chunks, compute, 0)

    for i in range(1, PLANE):
        loads_copy(i, beside(i)).wait_recv()
    loads_in[q] = loads[q]
    load_ref[...] = (jnp.sum(loads_in[...], axis=0) * load_scale)[:1, :1]

    def combine(c, carry):
        for i in range(1, PLANE):
            answer_copy(c, i, beside(i)).wait_recv()
        total = jnp.zeros((depth, width), jnp.float32)
        for k in range(PLANE):
            for half in range(2):
                total += jnp.dot(shares[k, half], inbox[c, k], preferred_element_type=jnp.float32)
        column[c] = total.reshape(column.shape[1:]).astype(jnp.bfloat16)
        for i in range(1, planes):
            sum_copy(c, i, p).start()
        sums_in[c, p] = column[c, p]
        return carry

    lax.fori_loop(0, chunks, combine, 0)

    def gather_sums(c, carry):
        for i in range(1, planes):
            sum_copy(c, i, along(i)).wait_recv()
        total = sums_in[c, 0].astype(jnp.float32)
        for k in range(1, planes):
            total += sums_in[c, k].astype(jnp.float32)
        out_ref[:, cut(c)] = total.astype(jnp.bfloat16)
        return carry

    lax.fori_loop(0, chunks, gather_sums, 0)

    for i in range(1, planes):
        notes_copy(i, p).wait_send()
    for i in range(1, PLANE):
        loads_copy(i, q).wait_send()

    def finish(c, carry):
        for i in range(1, PLANE):
            answer_copy(c, i, q).wait_send()
        for i in range(1, planes):
            x_copy(c, i, p).wait_send()
            sum_copy(c, i, p).wait_send()
        return carry

    lax.fori_loop(0, chunks, finish, 0)


def layer(x, ids, scores, gate, up, down, devices, tok_mb, capacity, load_scale):
    planes = devices // PLANE
    tokens, model_width = x.shape
    inner = gate.shape[1]
    width = next(w for w in (256, 128) if model_width % w == 0)
    chunks = model_width // width
    spots = planes * (tokens // tok_mb) * capacity
    dma = pltpu.SemaphoreType.DMA
    vmem = pl.BlockSpec(memory_space=pltpu.VMEM)
    hbm = pl.BlockSpec(memory_space=pl.ANY)
    bf16, f32 = jnp.bfloat16, jnp.float32
    return pl.pallas_call(
        functools.partial(layer_kernel, planes, capacity, tok_mb, load_scale),
        out_shape=(
            jax.ShapeDtypeStruct((tokens, model_width), bf16),
            jax.ShapeDtypeStruct((1, 1), f32),
        ),
        in_specs=[hbm, vmem, vmem, hbm, hbm, hbm],
        out_specs=(vmem, vmem),
        scratch_shapes=[
            pltpu.VMEM((tokens, model_width), bf16),
            pltpu.VMEM((planes, tokens // tok_mb, 2, ids.shape[1], 128), f32),
            pltpu.VMEM((chunks, planes, tokens, width), bf16),
            pltpu.VMEM((PLANE, spots, planes * tokens), bf16),
            pltpu.VMEM((PLANE, 2, planes * tokens, spots), bf16),
            pltpu.VMEM((chunks, PLANE, spots, width), bf16),
            pltpu.VMEM((chunks, PLANE, spots, width), bf16),
            pltpu.VMEM((PLANE, 8, 128), f32),
            pltpu.VMEM((PLANE, 8, 128), f32),
            pltpu.VMEM((SLOTS, width, inner), bf16),
            pltpu.VMEM((SLOTS, width, inner), bf16),
            pltpu.VMEM((chunks, inner, width), bf16),
            pltpu.VMEM((PLANE * spots, inner), f32),
            pltpu.VMEM((PLANE * spots, inner), f32),
            pltpu.VMEM((PLANE * spots, inner), bf16),
            pltpu.VMEM((chunks, PLANE, spots, width), bf16),
            pltpu.VMEM((chunks, planes, tokens, width), bf16),
            dma,
            dma((SLOTS,)),
            dma((SLOTS,)),
            dma((chunks,)),
            dma((planes,)),
            dma((planes,)),
            dma((chunks, planes)),
            dma((chunks, planes)),
            dma((PLANE,)),
            dma((PLANE,)),
            dma((chunks, PLANE)),
            dma((chunks, PLANE)),
            dma((chunks, PLANE)),
            dma((chunks, PLANE)),
            dma((chunks, planes)),
            dma((chunks, planes)),
        ],
        compiler_params=pltpu.CompilerParams(
            collective_id=0, has_side_effects=True, vmem_limit_bytes=66 * 1000 * 1000
        ),
    )(x, ids, scores, gate, up, down)


def shards(hidden, expert_ids, gate_scores, w_gate, w_up, w_down):
    devices = lax.axis_size("ep")
    micro_count, tok_mb, model_width = hidden.shape
    chosen = expert_ids.shape[2]
    capacity = tok_mb * chosen // devices + 1
    tokens = micro_count * tok_mb
    mixed, expert_load = layer(
        hidden.reshape(tokens, model_width),
        expert_ids.transpose(0, 2, 1),
        gate_scores.transpose(0, 2, 1),
        w_gate[0],
        w_up[0],
        w_down[0],
        devices,
        tok_mb,
        capacity,
        devices / (route_scale * tokens * devices),
    )
    return (mixed.reshape(micro_count, tok_mb, model_width), expert_load.reshape(1))


def solution(mesh):
    placed = (
        P(None, "ep", None),
        P(None, "ep", None),
        P(None, "ep", None),
        P("ep", None, None),
        P("ep", None, None),
        P("ep", None, None),
    )
    return jax.shard_map(
        shards,
        mesh=mesh,
        in_specs=placed,
        out_specs=(P(None, "ep", None), P("ep")),
        check_vma=False,
    )
```

```python
import functools

import jax
import jax.numpy as jnp
from jax import lax
from jax.experimental import pallas as pl
from jax.experimental.pallas import tpu as pltpu
from jax.sharding import PartitionSpec as P

route_scale = 2.5
PLANE = 8
SLOTS = 3
LAG = 3
MESH = pl.DeviceIdType.MESH


def tri(size, block):
    row = lax.broadcasted_iota(jnp.int32, (size, size), 0)
    col = lax.broadcasted_iota(jnp.int32, (size, size), 1)
    earlier = (row < col) & (lax.div(row, block) == lax.div(col, block))
    return jnp.where(earlier, 1.0, 0.0).astype(jnp.bfloat16)


def layer_kernel(
    planes,
    capacity,
    tok_mb,
    load_scale,
    hidden_ref,
    ids_ref,
    scores_ref,
    gate_ref,
    up_ref,
    down_ref,
    out_ref,
    load_ref,
    x_ref,
    notes,
    column,
    picks,
    shares,
    packed,
    rows,
    loads,
    loads_in,
    w_gate,
    w_up,
    w_down,
    acc_gate,
    acc_up,
    hid,
    inbox,
    sums_in,
    hidden_sem,
    gate_sem,
    up_sem,
    down_sem,
    n_send,
    n_recv,
    x_send,
    x_recv,
    l_send,
    l_recv,
    d_send,
    d_recv,
    a_send,
    a_recv,
    s_send,
    s_recv,
):
    me = lax.axis_index("ep")
    p = me // PLANE
    q = me % PLANE
    chunks, _, tokens, width = column.shape
    micro_count, chosen, _ = ids_ref.shape
    spots = packed.shape[2]
    depth = planes * tokens

    def cut(c):
        return pl.ds(pl.multiple_of(c * width, width), width)

    def load_in(c):
        slot = c % SLOTS
        return (
            pltpu.make_async_copy(gate_ref.at[cut(c), :], w_gate.at[slot], gate_sem.at[slot]),
            pltpu.make_async_copy(up_ref.at[cut(c), :], w_up.at[slot], up_sem.at[slot]),
        )

    load_down = pltpu.make_async_copy(down_ref, w_down, down_sem)

    hidden_copy = pltpu.make_async_copy(hidden_ref, x_ref, hidden_sem)
    hidden_copy.start()

    barrier = pltpu.get_barrier_semaphore()
    for i in range(1, PLANE):
        other = p * PLANE + (q + i) % PLANE
        pl.semaphore_signal(barrier, inc=1, device_id=(other,), device_id_type=MESH)
    for i in range(1, planes):
        other = ((p + i) % planes) * PLANE + q
        pl.semaphore_signal(barrier, inc=1, device_id=(other,), device_id_type=MESH)

    for c in range(SLOTS):
        for copy in load_in(c):
            copy.start()

    notes[p] = jnp.zeros(notes.shape[1:], jnp.float32)
    for m in range(micro_count):
        scores = scores_ref[m]
        notes[p, m, 0, :, :tok_mb] = ids_ref[m].astype(jnp.float32)
        notes[p, m, 1, :, :tok_mb] = route_scale * scores / jnp.sum(scores, axis=0, keepdims=True)
    hidden_copy.wait()

    pl.semaphore_wait(barrier, PLANE + planes - 2)

    def along(i):
        return (p + i) % planes

    def beside(i):
        return (q + i) % PLANE

    def up_down(src, dst, send, recv, i):
        return pltpu.make_async_remote_copy(
            src_ref=src,
            dst_ref=dst,
            send_sem=send,
            recv_sem=recv,
            device_id=(along(i) * PLANE + q,),
            device_id_type=MESH,
        )

    def across(src, dst, send, recv, i):
        return pltpu.make_async_remote_copy(
            src_ref=src,
            dst_ref=dst,
            send_sem=send,
            recv_sem=recv,
            device_id=(p * PLANE + beside(i),),
            device_id_type=MESH,
        )

    def notes_copy(i):
        return up_down(notes.at[p], notes.at[p], n_send, n_recv, i)

    def x_copy(c, i):
        return up_down(x_ref.at[:, cut(c)], column.at[c, p], x_send, x_recv.at[c], i)

    def loads_copy(i):
        return across(loads.at[beside(i)], loads_in.at[q], l_send, l_recv, i)

    def rows_copy(c, i):
        return across(packed.at[c, beside(i)], rows.at[c, q], d_send.at[c], d_recv.at[c], i)

    def answer_copy(c, i):
        return across(packed.at[c, beside(i)], inbox.at[c, q], a_send, a_recv.at[c], i)

    def sum_copy(c, i):
        return up_down(column.at[c, along(i)], sums_in.at[c, p], s_send, s_recv.at[c], i)

    def arrived(ref, sem):
        across(ref, ref, sem, sem, 1).wait_recv()

    def sent(ref, sem):
        across(ref, ref, sem, sem, 1).wait_send()

    for i in range(1, planes):
        notes_copy(i).start()

    def send_x(c, carry):
        for i in range(1, planes):
            x_copy(c, i).start()
        column[c, p] = x_ref[:, cut(c)]
        return carry

    lax.fori_loop(0, chunks, send_x, 0)

    load_down.start()
    arrived(notes.at[pl.ds(0, planes - 1)], n_recv)

    def spread(part):
        pieces = [notes[at, m, part] for at in range(planes) for m in range(micro_count)]
        lanes = []
        for at in range(0, len(pieces), 128 // tok_mb):
            block = pieces[at]
            for k, piece in enumerate(pieces[at + 1 : at + 128 // tok_mb]):
                block += pltpu.roll(piece, (k + 1) * tok_mb, 1)
            lanes.append(block)
        return jnp.concatenate(lanes, axis=1)

    ids, weights = spread(0), spread(1)
    expert = (p * PLANE + lax.broadcasted_iota(jnp.int32, (PLANE, depth), 0)).astype(jnp.float32)
    named = jnp.zeros((PLANE, depth), jnp.float32)
    share = jnp.zeros((PLANE, depth), jnp.float32)
    for k in range(chosen):
        same = jnp.broadcast_to(ids[k : k + 1], (PLANE, depth)) == expert
        named += jnp.where(same, 1.0, 0.0)
        share += jnp.where(same, jnp.broadcast_to(weights[k : k + 1], (PLANE, depth)), 0.0)
    for j in range(PLANE):
        own = jnp.sum(share[j : j + 1], axis=1, keepdims=True)
        loads[j] = jnp.broadcast_to(own, loads.shape[1:])
    for i in range(1, PLANE):
        loads_copy(i).start()

    earlier = tri(128, tok_mb)
    rank = jnp.concatenate(
        [
            jnp.dot(
                named[:, at : at + 128].astype(jnp.bfloat16),
                earlier,
                preferred_element_type=jnp.float32,
            )
            for at in range(0, depth, 128)
        ],
        axis=1,
    )
    start = lax.div(lax.broadcasted_iota(jnp.int32, (PLANE, depth), 1), tok_mb) * capacity
    spot = jnp.where(named > 0.5, start.astype(jnp.float32) + rank, -1.0)
    place = lax.broadcasted_iota(jnp.int32, (spots, depth), 0).astype(jnp.float32)
    for j in range(PLANE):
        found = place == jnp.broadcast_to(spot[j : j + 1], (spots, depth))
        picks[j] = jnp.where(found, 1.0, 0.0).astype(jnp.bfloat16)

    def dispatch(c):
        arrived(column.at[c, pl.ds(0, planes - 1)], x_recv.at[c])
        tokens_here = column[c].reshape(depth, width)
        found = jnp.dot(
            picks[...].reshape(PLANE * spots, depth),
            tokens_here,
            preferred_element_type=jnp.float32,
        )
        packed[c] = found.reshape(packed.shape[1:]).astype(jnp.bfloat16)
        for i in range(1, PLANE):
            rows_copy(c, i).start()
        rows[c, q] = packed[c, q]

    def consume(c):
        for copy in load_in(c):
            copy.wait()
        arrived(rows.at[c, pl.ds(0, PLANE - 1)], d_recv.at[c])
        slot = c % SLOTS
        got = rows[c].reshape(PLANE * spots, width)
        acc_gate[...] += jnp.dot(got, w_gate[slot], preferred_element_type=jnp.float32)
        acc_up[...] += jnp.dot(got, w_up[slot], preferred_element_type=jnp.float32)

        @pl.when(c + SLOTS < chunks)
        def _():
            for copy in load_in(c + SLOTS):
                copy.start()

    acc_gate[...] = jnp.zeros(acc_gate.shape, jnp.float32)
    acc_up[...] = jnp.zeros(acc_up.shape, jnp.float32)

    def step(c, carry):
        pl.when(c < chunks)(lambda: dispatch(c))
        pl.when(c >= LAG)(lambda: consume(c - LAG))
        return carry

    lax.fori_loop(0, LAG, step, 0)

    both = jnp.concatenate(
        [spot, share, jnp.zeros((128 - 2 * PLANE, depth), jnp.float32)], axis=0
    ).T
    lane = lax.broadcasted_iota(jnp.int32, (depth, 128), 1).astype(jnp.float32)
    for j in range(PLANE):
        found = lane == jnp.broadcast_to(both[:, j : j + 1], (depth, 128))
        held = jnp.broadcast_to(both[:, PLANE + j : PLANE + j + 1], (depth, 128))
        held = jnp.where(found, held, 0.0)
        high = held.astype(jnp.bfloat16)
        shares[j, 0] = high[:, :spots]
        shares[j, 1] = (held - high.astype(jnp.float32)).astype(jnp.bfloat16)[:, :spots]

    lax.fori_loop(LAG, chunks + LAG, step, 0)

    gate = acc_gate[...]
    hid[...] = (gate / (1.0 + jnp.exp(-gate)) * acc_up[...]).astype(jnp.bfloat16)

    load_down.wait()

    def compute(c, carry):
        sent(packed.at[c, pl.ds(0, PLANE - 1)], d_send.at[c])
        found = jnp.dot(hid[...], w_down[:, cut(c)], preferred_element_type=jnp.float32)
        packed[c] = found.reshape(packed.shape[1:]).astype(jnp.bfloat16)
        for i in range(1, PLANE):
            answer_copy(c, i).start()
        inbox[c, q] = packed[c, q]
        return carry

    lax.fori_loop(0, chunks, compute, 0)

    arrived(loads_in.at[pl.ds(0, PLANE - 1)], l_recv)
    loads_in[q] = loads[q]
    load_ref[...] = (jnp.sum(loads_in[...], axis=0) * load_scale)[:1, :1]

    def combine(c, carry):
        arrived(inbox.at[c, pl.ds(0, PLANE - 1)], a_recv.at[c])
        total = jnp.zeros((depth, width), jnp.float32)
        for k in range(PLANE):
            for half in range(2):
                total += jnp.dot(shares[k, half], inbox[c, k], preferred_element_type=jnp.float32)
        column[c] = total.reshape(column.shape[1:]).astype(jnp.bfloat16)
        for i in range(1, planes):
            sum_copy(c, i).start()
        sums_in[c, p] = column[c, p]
        return carry

    lax.fori_loop(0, chunks, combine, 0)

    def gather_sums(c, carry):
        arrived(sums_in.at[c, pl.ds(0, planes - 1)], s_recv.at[c])
        total = sums_in[c, 0].astype(jnp.float32)
        for k in range(1, planes):
            total += sums_in[c, k].astype(jnp.float32)
        out_ref[:, cut(c)] = total.astype(jnp.bfloat16)
        return carry

    lax.fori_loop(0, chunks, gather_sums, 0)

    sent(notes.at[pl.ds(0, planes - 1)], n_send)
    sent(loads.at[pl.ds(0, PLANE - 1)], l_send)
    sent(column.at[:, pl.ds(0, planes - 1)], x_send)
    sent(column.at[:, pl.ds(0, planes - 1)], s_send)
    sent(packed.at[:, pl.ds(0, PLANE - 1)], a_send)


def layer(x, ids, scores, gate, up, down, devices, tok_mb, capacity, load_scale):
    planes = devices // PLANE
    tokens, model_width = x.shape
    inner = gate.shape[1]
    width = next(w for w in (256, 128) if model_width % w == 0)
    chunks = model_width // width
    spots = planes * (tokens // tok_mb) * capacity
    dma = pltpu.SemaphoreType.DMA
    vmem = pl.BlockSpec(memory_space=pltpu.VMEM)
    hbm = pl.BlockSpec(memory_space=pl.ANY)
    bf16, f32 = jnp.bfloat16, jnp.float32
    return pl.pallas_call(
        functools.partial(layer_kernel, planes, capacity, tok_mb, load_scale),
        out_shape=(
            jax.ShapeDtypeStruct((tokens, model_width), bf16),
            jax.ShapeDtypeStruct((1, 1), f32),
        ),
        in_specs=[hbm, vmem, vmem, hbm, hbm, hbm],
        out_specs=(vmem, vmem),
        scratch_shapes=[
            pltpu.VMEM((tokens, model_width), bf16),
            pltpu.VMEM((planes, tokens // tok_mb, 2, ids.shape[1], 128), f32),
            pltpu.VMEM((chunks, planes, tokens, width), bf16),
            pltpu.VMEM((PLANE, spots, planes * tokens), bf16),
            pltpu.VMEM((PLANE, 2, planes * tokens, spots), bf16),
            pltpu.VMEM((chunks, PLANE, spots, width), bf16),
            pltpu.VMEM((chunks, PLANE, spots, width), bf16),
            pltpu.VMEM((PLANE, 8, 128), f32),
            pltpu.VMEM((PLANE, 8, 128), f32),
            pltpu.VMEM((SLOTS, width, inner), bf16),
            pltpu.VMEM((SLOTS, width, inner), bf16),
            pltpu.VMEM((inner, model_width), bf16),
            pltpu.VMEM((PLANE * spots, inner), f32),
            pltpu.VMEM((PLANE * spots, inner), f32),
            pltpu.VMEM((PLANE * spots, inner), bf16),
            pltpu.VMEM((chunks, PLANE, spots, width), bf16),
            pltpu.VMEM((chunks, planes, tokens, width), bf16),
            dma,
            dma((SLOTS,)),
            dma((SLOTS,)),
            dma,
            dma,
            dma,
            dma,
            dma((chunks,)),
            dma,
            dma,
            dma((chunks,)),
            dma((chunks,)),
            dma,
            dma((chunks,)),
            dma,
            dma((chunks,)),
        ],
        compiler_params=pltpu.CompilerParams(
            collective_id=0, has_side_effects=True, vmem_limit_bytes=66 * 1000 * 1000
        ),
    )(x, ids, scores, gate, up, down)


def shards(hidden, expert_ids, gate_scores, w_gate, w_up, w_down):
    devices = lax.axis_size("ep")
    micro_count, tok_mb, model_width = hidden.shape
    chosen = expert_ids.shape[2]
    capacity = tok_mb * chosen // devices + 1
    tokens = micro_count * tok_mb
    mixed, expert_load = layer(
        hidden.reshape(tokens, model_width),
        expert_ids.transpose(0, 2, 1),
        gate_scores.transpose(0, 2, 1),
        w_gate[0],
        w_up[0],
        w_down[0],
        devices,
        tok_mb,
        capacity,
        devices / (route_scale * tokens * devices),
    )
    return (mixed.reshape(micro_count, tok_mb, model_width), expert_load.reshape(1))


def solution(mesh):
    placed = (
        P(None, "ep", None),
        P(None, "ep", None),
        P(None, "ep", None),
        P("ep", None, None),
        P("ep", None, None),
        P("ep", None, None),
    )
    return jax.shard_map(
        shards,
        mesh=mesh,
        in_specs=placed,
        out_specs=(P(None, "ep", None), P("ep")),
        check_vma=False,
    )
```

```python
import functools

import jax
import jax.numpy as jnp
from jax import lax
from jax.experimental import pallas as pl
from jax.experimental.pallas import tpu as pltpu
from jax.sharding import PartitionSpec as P

route_scale = 2.5
PLANE = 8
SLOTS = 3
LAG = 3
QUADS = PLANE // 2
FLIPPED = 2
MESH = pl.DeviceIdType.MESH


class Route:
    def __init__(self, gather_at, gather_of, scatter_at, scatter_of, notes, picks, shares):
        self.gather_at, self.gather_of = gather_at, gather_of
        self.scatter_at, self.scatter_of = scatter_at, scatter_of
        self.notes, self.picks, self.shares = notes, picks, shares


def tri(size, block):
    row = lax.broadcasted_iota(jnp.int32, (size, size), 0)
    col = lax.broadcasted_iota(jnp.int32, (size, size), 1)
    earlier = (row < col) & (lax.div(row, block) == lax.div(col, block))
    return jnp.where(earlier, 1.0, 0.0).astype(jnp.bfloat16)


def layer_kernel(
    planes,
    capacity,
    tok_mb,
    load_scale,
    flipped,
    hidden_ref,
    ids_ref,
    scores_ref,
    gate_ref,
    up_ref,
    down_ref,
    out_ref,
    load_ref,
    x_ref,
    notes,
    column,
    picks,
    shares,
    notes_f,
    picks_f,
    shares_f,
    perm,
    packed,
    rows,
    loads,
    loads_in,
    w_gate,
    w_up,
    w_down,
    acc_gate,
    acc_up,
    hid,
    inbox,
    sums_in,
    hidden_sem,
    gate_sem,
    up_sem,
    down_sem,
    n_send,
    n_recv,
    f_send,
    f_recv,
    x_send,
    x_recv,
    l_send,
    l_recv,
    d_send,
    d_recv,
    a_send,
    a_recv,
    s_send,
    s_recv,
):
    me = lax.axis_index("ep")
    p = me // PLANE
    q = me % PLANE
    quad, core = q // 2, q % 2
    chunks, _, tokens, width = column.shape
    micro_count, chosen, _ = ids_ref.shape
    spots = packed.shape[2]
    depth = planes * tokens
    straight = chunks - flipped

    def cut(c):
        return pl.ds(pl.multiple_of(c * width, width), width)

    def load_in(c):
        slot = c % SLOTS
        return (
            pltpu.make_async_copy(gate_ref.at[cut(c), :], w_gate.at[slot], gate_sem.at[slot]),
            pltpu.make_async_copy(up_ref.at[cut(c), :], w_up.at[slot], up_sem.at[slot]),
        )

    load_down = pltpu.make_async_copy(down_ref, w_down, down_sem)

    hidden_copy = pltpu.make_async_copy(hidden_ref, x_ref, hidden_sem)
    hidden_copy.start()

    turn = p * 2 + core
    ahead = Route(
        p,
        lambda i: ((p + i) % planes, ((p + i) % planes) * PLANE + q),
        q,
        lambda i: ((q + i) % PLANE, p * PLANE + (q + i) % PLANE),
        notes,
        picks,
        shares,
    )
    aside = Route(
        quad,
        lambda i: ((quad + i) % QUADS, p * PLANE + ((quad + i) % QUADS) * 2 + core),
        turn,
        lambda i: (
            (turn + i) % (2 * planes),
            ((turn + i) % (2 * planes)) // 2 * PLANE + quad * 2 + (turn + i) % 2,
        ),
        notes_f,
        picks_f,
        shares_f,
    )

    barrier = pltpu.get_barrier_semaphore()

    def greet(other):
        pl.semaphore_signal(barrier, inc=1, device_id=(other,), device_id_type=MESH)

    for i in range(1, PLANE):
        greet(ahead.scatter_of(i)[1])
    for i in range(1, planes):
        greet(ahead.gather_of(i)[1])
    if flipped:
        for i in range(1, planes):
            greet(((p + i) % planes) * PLANE + quad * 2 + 1 - core)

    for c in range(SLOTS):
        for copy in load_in(c):
            copy.start()

    notes[p] = jnp.zeros(notes.shape[1:], jnp.float32)
    for m in range(micro_count):
        scores = scores_ref[m]
        notes[p, m, 0, :, :tok_mb] = ids_ref[m].astype(jnp.float32)
        notes[p, m, 1, :, :tok_mb] = route_scale * scores / jnp.sum(scores, axis=0, keepdims=True)
    if flipped:
        notes_f[quad] = notes[p]
    hidden_copy.wait()

    pl.semaphore_wait(barrier, PLANE + planes - 2 + (planes - 1 if flipped else 0))

    def remote(src, dst, send, recv, other):
        return pltpu.make_async_remote_copy(
            src_ref=src,
            dst_ref=dst,
            send_sem=send,
            recv_sem=recv,
            device_id=(other,),
            device_id_type=MESH,
        )

    def notes_copy(way, i, send, recv):
        mine = way.notes.at[way.gather_at]
        return remote(mine, mine, send, recv, way.gather_of(i)[1])

    def x_copy(way, c, i):
        place = column.at[c, way.gather_at]
        return remote(x_ref.at[:, cut(c)], place, x_send, x_recv.at[c], way.gather_of(i)[1])

    def loads_copy(i):
        at, other = ahead.scatter_of(i)
        return remote(loads.at[at], loads_in.at[q], l_send, l_recv, other)

    def rows_copy(way, c, i):
        at, other = way.scatter_of(i)
        place = rows.at[c, way.scatter_at]
        return remote(packed.at[c, at], place, d_send.at[c], d_recv.at[c], other)

    def answer_copy(way, c, i):
        at, other = way.scatter_of(i)
        place = inbox.at[c, way.scatter_at]
        return remote(packed.at[c, at], place, a_send, a_recv.at[c], other)

    def sum_copy(way, c, i):
        at, other = way.gather_of(i)
        place = sums_in.at[c, way.gather_at]
        return remote(column.at[c, at], place, s_send, s_recv.at[c], other)

    def arrived(ref, sem):
        remote(ref, ref, sem, sem, ahead.scatter_of(1)[1]).wait_recv()

    def sent(ref, sem):
        remote(ref, ref, sem, sem, ahead.scatter_of(1)[1]).wait_send()

    for i in range(1, planes):
        notes_copy(ahead, i, n_send, n_recv).start()

    def send_x(way, c):
        for i in range(1, planes):
            x_copy(way, c, i).start()
        column[c, way.gather_at] = x_ref[:, cut(c)]

    def send_ahead(c, carry):
        send_x(ahead, c)
        return carry

    if flipped:
        for i in range(1, QUADS):
            notes_copy(aside, i, f_send, f_recv).start()
        for c in range(straight, chunks):
            send_x(aside, c)
    lax.fori_loop(0, straight, send_ahead, 0)

    load_down.start()
    arrived(notes.at[pl.ds(0, planes - 1)], n_recv)

    earlier = tri(128, tok_mb)

    def spread(way, part):
        pieces = [way.notes[at, m, part] for at in range(planes) for m in range(micro_count)]
        lanes = []
        for at in range(0, len(pieces), 128 // tok_mb):
            block = pieces[at]
            for k, piece in enumerate(pieces[at + 1 : at + 128 // tok_mb]):
                block += pltpu.roll(piece, (k + 1) * tok_mb, 1)
            lanes.append(block)
        return jnp.concatenate(lanes, axis=1)

    def prepare(way, expert):
        ids, weights = spread(way, 0), spread(way, 1)
        named = jnp.zeros((PLANE, depth), jnp.float32)
        share = jnp.zeros((PLANE, depth), jnp.float32)
        for k in range(chosen):
            same = jnp.broadcast_to(ids[k : k + 1], (PLANE, depth)) == expert
            named += jnp.where(same, 1.0, 0.0)
            share += jnp.where(same, jnp.broadcast_to(weights[k : k + 1], (PLANE, depth)), 0.0)
        rank = jnp.concatenate(
            [
                jnp.dot(
                    named[:, at : at + 128].astype(jnp.bfloat16),
                    earlier,
                    preferred_element_type=jnp.float32,
                )
                for at in range(0, depth, 128)
            ],
            axis=1,
        )
        start = lax.div(lax.broadcasted_iota(jnp.int32, (PLANE, depth), 1), tok_mb) * capacity
        spot = jnp.where(named > 0.5, start.astype(jnp.float32) + rank, -1.0)
        place = lax.broadcasted_iota(jnp.int32, (spots, depth), 0).astype(jnp.float32)
        for j in range(PLANE):
            found = place == jnp.broadcast_to(spot[j : j + 1], (spots, depth))
            way.picks[j] = jnp.where(found, 1.0, 0.0).astype(jnp.bfloat16)
        return spot, share

    def weigh(way, spot, share):
        both = jnp.concatenate(
            [spot, share, jnp.zeros((128 - 2 * PLANE, depth), jnp.float32)], axis=0
        ).T
        lane = lax.broadcasted_iota(jnp.int32, (depth, 128), 1).astype(jnp.float32)
        for j in range(PLANE):
            found = lane == jnp.broadcast_to(both[:, j : j + 1], (depth, 128))
            held = jnp.broadcast_to(both[:, PLANE + j : PLANE + j + 1], (depth, 128))
            held = jnp.where(found, held, 0.0)
            high = held.astype(jnp.bfloat16)
            way.shares[j, 0] = high[:, :spots]
            way.shares[j, 1] = (held - high.astype(jnp.float32)).astype(jnp.bfloat16)[:, :spots]

    index = lax.broadcasted_iota(jnp.int32, (PLANE, depth), 0)
    spot, share = prepare(ahead, (p * PLANE + index).astype(jnp.float32))
    for j in range(PLANE):
        own = jnp.sum(share[j : j + 1], axis=1, keepdims=True)
        loads[j] = jnp.broadcast_to(own, loads.shape[1:])
    for i in range(1, PLANE):
        loads_copy(i).start()

    def dispatch(way, c):
        arrived(column.at[c, pl.ds(0, planes - 1)], x_recv.at[c])
        tokens_here = column[c].reshape(depth, width)
        found = jnp.dot(
            way.picks[...].reshape(PLANE * spots, depth),
            tokens_here,
            preferred_element_type=jnp.float32,
        )
        packed[c] = found.reshape(packed.shape[1:]).astype(jnp.bfloat16)
        for i in range(1, PLANE):
            rows_copy(way, c, i).start()
        rows[c, way.scatter_at] = packed[c, way.scatter_at]

    def reorder(values):
        return jnp.dot(perm[...], values, preferred_element_type=jnp.float32).astype(jnp.bfloat16)

    def consume(way, c):
        for copy in load_in(c):
            copy.wait()
        arrived(rows.at[c, pl.ds(0, PLANE - 1)], d_recv.at[c])
        slot = c % SLOTS
        got = rows[c].reshape(PLANE * spots, width)
        if way is aside:
            got = reorder(got)
        acc_gate[...] += jnp.dot(got, w_gate[slot], preferred_element_type=jnp.float32)
        acc_up[...] += jnp.dot(got, w_up[slot], preferred_element_type=jnp.float32)

        @pl.when(c + SLOTS < chunks)
        def _():
            for copy in load_in(c + SLOTS):
                copy.start()

    def step(c, carry):
        pl.when(c < straight)(lambda: dispatch(ahead, c))
        pl.when(c >= LAG)(lambda: consume(ahead, c - LAG))
        return carry

    lax.fori_loop(0, LAG, step, 0)

    acc_gate[...] = jnp.zeros(acc_gate.shape, jnp.float32)
    acc_up[...] = jnp.zeros(acc_up.shape, jnp.float32)
    if flipped:
        arrived(notes_f.at[pl.ds(0, QUADS - 1)], f_recv)
        expert = lax.div(index, 2) * PLANE + quad * 2 + lax.rem(index, 2)
        spot_f, share_f = prepare(aside, expert.astype(jnp.float32))
        for c in range(straight, chunks):
            dispatch(aside, c)
        weigh(aside, spot_f, share_f)
        size = perm.shape[0]
        held = spots // planes
        row = lax.broadcasted_iota(jnp.int32, (size, 128), 0)
        group = lax.div(row, held)
        at_plane, at_core, at_quad = lax.rem(group, planes), lax.rem(lax.div(group, planes), 2), lax.div(group, 2 * planes)
        target = (at_plane * PLANE + at_core * QUADS + at_quad) * held + lax.rem(row, held)
        for at in range(0, size, 128):
            lane = at + lax.broadcasted_iota(jnp.int32, (size, 128), 1)
            block = jnp.where(lane == target, 1.0, 0.0).astype(jnp.bfloat16)
            perm[:, at : min(at + 128, size)] = block[:, : min(128, size - at)]
    weigh(ahead, spot, share)

    lax.fori_loop(LAG, straight + LAG, step, 0)
    for c in range(straight, chunks):
        consume(aside, c)

    gate = acc_gate[...]
    hid[...] = (gate / (1.0 + jnp.exp(-gate)) * acc_up[...]).astype(jnp.bfloat16)

    load_down.wait()

    def compute(way, c):
        sent(packed.at[c, pl.ds(0, PLANE - 1)], d_send.at[c])
        found = jnp.dot(hid[...], w_down[:, cut(c)], preferred_element_type=jnp.float32)
        if way is aside:
            found = jnp.dot(
                perm[...], found.astype(jnp.bfloat16), preferred_element_type=jnp.float32
            )
        packed[c] = found.reshape(packed.shape[1:]).astype(jnp.bfloat16)
        for i in range(1, PLANE):
            answer_copy(way, c, i).start()
        inbox[c, way.scatter_at] = packed[c, way.scatter_at]

    def compute_ahead(c, carry):
        compute(ahead, c)
        return carry

    first = min(2, straight)
    lax.fori_loop(0, first, compute_ahead, 0)
    for c in range(straight, chunks):
        compute(aside, c)
    lax.fori_loop(first, straight, compute_ahead, 0)

    arrived(loads_in.at[pl.ds(0, PLANE - 1)], l_recv)
    loads_in[q] = loads[q]
    load_ref[...] = (jnp.sum(loads_in[...], axis=0) * load_scale)[:1, :1]

    def combine(way, c):
        arrived(inbox.at[c, pl.ds(0, PLANE - 1)], a_recv.at[c])
        total = jnp.zeros((depth, width), jnp.float32)
        for k in range(PLANE):
            for half in range(2):
                total += jnp.dot(
                    way.shares[k, half], inbox[c, k], preferred_element_type=jnp.float32
                )
        column[c] = total.reshape(column.shape[1:]).astype(jnp.bfloat16)
        for i in range(1, planes):
            sum_copy(way, c, i).start()
        sums_in[c, way.gather_at] = column[c, way.gather_at]

    def combine_ahead(c, carry):
        combine(ahead, c)
        return carry

    lax.fori_loop(0, straight, combine_ahead, 0)
    for c in range(straight, chunks):
        combine(aside, c)

    def gather_sums(c, carry):
        arrived(sums_in.at[c, pl.ds(0, planes - 1)], s_recv.at[c])
        total = sums_in[c, 0].astype(jnp.float32)
        for k in range(1, planes):
            total += sums_in[c, k].astype(jnp.float32)
        out_ref[:, cut(c)] = total.astype(jnp.bfloat16)
        return carry

    lax.fori_loop(0, chunks, gather_sums, 0)

    sent(notes.at[pl.ds(0, planes - 1)], n_send)
    if flipped:
        sent(notes_f.at[pl.ds(0, QUADS - 1)], f_send)
    sent(loads.at[pl.ds(0, PLANE - 1)], l_send)
    sent(column.at[:, pl.ds(0, planes - 1)], x_send)
    sent(column.at[:, pl.ds(0, planes - 1)], s_send)
    sent(packed.at[:, pl.ds(0, PLANE - 1)], a_send)


def layer(x, ids, scores, gate, up, down, devices, tok_mb, capacity, load_scale):
    planes = devices // PLANE
    tokens, model_width = x.shape
    inner = gate.shape[1]
    width = next(w for w in (256, 128) if model_width % w == 0)
    chunks = model_width // width
    spots = planes * (tokens // tok_mb) * capacity
    flipped = FLIPPED if planes == QUADS else 0
    few = (lambda *shape: shape) if flipped else (lambda *shape: (1,) * len(shape))
    dma = pltpu.SemaphoreType.DMA
    vmem = pl.BlockSpec(memory_space=pltpu.VMEM)
    hbm = pl.BlockSpec(memory_space=pl.ANY)
    bf16, f32 = jnp.bfloat16, jnp.float32
    return pl.pallas_call(
        functools.partial(layer_kernel, planes, capacity, tok_mb, load_scale, flipped),
        out_shape=(
            jax.ShapeDtypeStruct((tokens, model_width), bf16),
            jax.ShapeDtypeStruct((1, 1), f32),
        ),
        in_specs=[hbm, vmem, vmem, hbm, hbm, hbm],
        out_specs=(vmem, vmem),
        scratch_shapes=[
            pltpu.VMEM((tokens, model_width), bf16),
            pltpu.VMEM((planes, tokens // tok_mb, 2, ids.shape[1], 128), f32),
            pltpu.VMEM((chunks, planes, tokens, width), bf16),
            pltpu.VMEM((PLANE, spots, planes * tokens), bf16),
            pltpu.VMEM((PLANE, 2, planes * tokens, spots), bf16),
            pltpu.VMEM(few(planes, tokens // tok_mb, 2, ids.shape[1], 128), f32),
            pltpu.VMEM(few(PLANE, spots, planes * tokens), bf16),
            pltpu.VMEM(few(PLANE, 2, planes * tokens, spots), bf16),
            pltpu.VMEM(few(PLANE * spots, PLANE * spots), bf16),
            pltpu.VMEM((chunks, PLANE, spots, width), bf16),
            pltpu.VMEM((chunks, PLANE, spots, width), bf16),
            pltpu.VMEM((PLANE, 8, 128), f32),
            pltpu.VMEM((PLANE, 8, 128), f32),
            pltpu.VMEM((SLOTS, width, inner), bf16),
            pltpu.VMEM((SLOTS, width, inner), bf16),
            pltpu.VMEM((inner, model_width), bf16),
            pltpu.VMEM((PLANE * spots, inner), f32),
            pltpu.VMEM((PLANE * spots, inner), f32),
            pltpu.VMEM((PLANE * spots, inner), bf16),
            pltpu.VMEM((chunks, PLANE, spots, width), bf16),
            pltpu.VMEM((chunks, planes, tokens, width), bf16),
            dma,
            dma((SLOTS,)),
            dma((SLOTS,)),
            dma,
            dma,
            dma,
            dma,
            dma,
            dma,
            dma((chunks,)),
            dma,
            dma,
            dma((chunks,)),
            dma((chunks,)),
            dma,
            dma((chunks,)),
            dma,
            dma((chunks,)),
        ],
        compiler_params=pltpu.CompilerParams(
            collective_id=0, has_side_effects=True, vmem_limit_bytes=66 * 1000 * 1000
        ),
    )(x, ids, scores, gate, up, down)


def shards(hidden, expert_ids, gate_scores, w_gate, w_up, w_down):
    devices = lax.axis_size("ep")
    micro_count, tok_mb, model_width = hidden.shape
    chosen = expert_ids.shape[2]
    capacity = tok_mb * chosen // devices + 1
    tokens = micro_count * tok_mb
    mixed, expert_load = layer(
        hidden.reshape(tokens, model_width),
        expert_ids.transpose(0, 2, 1),
        gate_scores.transpose(0, 2, 1),
        w_gate[0],
        w_up[0],
        w_down[0],
        devices,
        tok_mb,
        capacity,
        devices / (route_scale * tokens * devices),
    )
    return (mixed.reshape(micro_count, tok_mb, model_width), expert_load.reshape(1))


def solution(mesh):
    placed = (
        P(None, "ep", None),
        P(None, "ep", None),
        P(None, "ep", None),
        P("ep", None, None),
        P("ep", None, None),
        P("ep", None, None),
    )
    return jax.shard_map(
        shards,
        mesh=mesh,
        in_specs=placed,
        out_specs=(P(None, "ep", None), P("ep")),
        check_vma=False,
    )
```

```python
import functools

import jax
import jax.numpy as jnp
from jax import lax
from jax.experimental import pallas as pl
from jax.experimental.pallas import tpu as pltpu
from jax.sharding import PartitionSpec as P

route_scale = 2.5
PLANE = 8
SLOTS = 3
LAG = 3
AHEAD = 3
ASIDE = (5, 8)
QUADS = PLANE // 2
FLIPPED = 2
MESH = pl.DeviceIdType.MESH


class Route:
    def __init__(self, gather_at, gather_of, scatter_at, scatter_of, notes, picks, shares):
        self.gather_at, self.gather_of = gather_at, gather_of
        self.scatter_at, self.scatter_of = scatter_at, scatter_of
        self.notes, self.picks, self.shares = notes, picks, shares


def tri(size, block):
    row = lax.broadcasted_iota(jnp.int32, (size, size), 0)
    col = lax.broadcasted_iota(jnp.int32, (size, size), 1)
    earlier = (row < col) & (lax.div(row, block) == lax.div(col, block))
    return jnp.where(earlier, 1.0, 0.0).astype(jnp.bfloat16)


def layer_kernel(
    planes,
    capacity,
    tok_mb,
    load_scale,
    flipped,
    hidden_ref,
    ids_ref,
    scores_ref,
    gate_ref,
    up_ref,
    down_ref,
    out_ref,
    load_ref,
    x_ref,
    notes,
    column,
    picks,
    shares,
    notes_f,
    picks_f,
    shares_f,
    perm,
    packed,
    rows,
    loads,
    loads_in,
    w_gate,
    w_up,
    w_down,
    acc_gate,
    acc_up,
    hid,
    inbox,
    sums_in,
    hidden_sem,
    gate_sem,
    up_sem,
    down_sem,
    n_send,
    n_recv,
    f_send,
    f_recv,
    x_far,
    s_far,
    x_send,
    x_recv,
    l_send,
    l_recv,
    d_send,
    d_recv,
    a_send,
    a_recv,
    s_send,
    s_recv,
):
    me = lax.axis_index("ep")
    p = me // PLANE
    q = me % PLANE
    quad, core = q // 2, q % 2
    chunks, _, tokens, width = column.shape
    micro_count, chosen, _ = ids_ref.shape
    spots = packed.shape[2]
    depth = planes * tokens
    straight = chunks - flipped

    def cut(c):
        return pl.ds(pl.multiple_of(c * width, width), width)

    def load_in(c):
        slot = c % SLOTS
        return (
            pltpu.make_async_copy(gate_ref.at[cut(c), :], w_gate.at[slot], gate_sem.at[slot]),
            pltpu.make_async_copy(up_ref.at[cut(c), :], w_up.at[slot], up_sem.at[slot]),
        )

    load_down = pltpu.make_async_copy(down_ref, w_down, down_sem)

    hidden_copy = pltpu.make_async_copy(hidden_ref, x_ref, hidden_sem)
    hidden_copy.start()

    turn = p * 2 + core
    ahead = Route(
        p,
        lambda i: ((p + i) % planes, ((p + i) % planes) * PLANE + q),
        q,
        lambda i: ((q + i) % PLANE, p * PLANE + (q + i) % PLANE),
        notes,
        picks,
        shares,
    )
    aside = Route(
        quad,
        lambda i: ((quad + i) % QUADS, p * PLANE + ((quad + i) % QUADS) * 2 + core),
        turn,
        lambda i: (
            (turn + i) % (2 * planes),
            ((turn + i) % (2 * planes)) // 2 * PLANE + quad * 2 + (turn + i) % 2,
        ),
        notes_f,
        picks_f,
        shares_f,
    )

    near = p + 1 - 2 * (p % 2)
    far = (p + 2) % planes
    last = (near + 2) % planes

    barrier = pltpu.get_barrier_semaphore()

    def greet(other):
        pl.semaphore_signal(barrier, inc=1, device_id=(other,), device_id_type=MESH)

    for i in range(1, PLANE):
        greet(ahead.scatter_of(i)[1])
    for i in range(1, planes):
        greet(ahead.gather_of(i)[1])
    if flipped:
        for i in range(1, planes):
            greet(((p + i) % planes) * PLANE + quad * 2 + 1 - core)

    for c in range(SLOTS):
        for copy in load_in(c):
            copy.start()

    notes[p] = jnp.zeros(notes.shape[1:], jnp.float32)
    for m in range(micro_count):
        scores = scores_ref[m]
        notes[p, m, 0, :, :tok_mb] = ids_ref[m].astype(jnp.float32)
        notes[p, m, 1, :, :tok_mb] = route_scale * scores / jnp.sum(scores, axis=0, keepdims=True)
    if flipped:
        notes_f[quad] = notes[p]
    hidden_copy.wait()

    pl.semaphore_wait(barrier, PLANE + planes - 2 + (planes - 1 if flipped else 0))

    def remote(src, dst, send, recv, other):
        return pltpu.make_async_remote_copy(
            src_ref=src,
            dst_ref=dst,
            send_sem=send,
            recv_sem=recv,
            device_id=(other,),
            device_id_type=MESH,
        )

    def notes_copy(way, i, send, recv):
        mine = way.notes.at[way.gather_at]
        return remote(mine, mine, send, recv, way.gather_of(i)[1])

    def x_copy(way, c, i):
        place = column.at[c, way.gather_at]
        return remote(x_ref.at[:, cut(c)], place, x_send, x_recv.at[c], way.gather_of(i)[1])

    def loads_copy(i):
        at, other = ahead.scatter_of(i)
        return remote(loads.at[at], loads_in.at[q], l_send, l_recv, other)

    def rows_copy(way, c, i):
        at, other = way.scatter_of(i)
        place = rows.at[c, way.scatter_at]
        return remote(packed.at[c, at], place, d_send.at[c], d_recv.at[c], other)

    def answer_copy(way, c, i):
        at, other = way.scatter_of(i)
        place = inbox.at[c, way.scatter_at]
        return remote(packed.at[c, at], place, a_send, a_recv.at[c], other)

    def sum_copy(way, c, i):
        at, other = way.gather_of(i)
        place = sums_in.at[c, way.gather_at]
        return remote(column.at[c, at], place, s_send, s_recv.at[c], other)

    def column_dev(at):
        return at * PLANE + q

    def x_first(c):
        place = column.at[c, p]
        mine = x_ref.at[:, cut(c)]
        return (
            remote(mine, place, x_send, x_recv.at[c], column_dev(near)),
            remote(mine, place, x_send, x_far.at[c], column_dev(far)),
        )

    def x_relay(c):
        place = column.at[c, far]
        return remote(place, place, x_send, x_recv.at[c], column_dev(near))

    def sum_first(c):
        return tuple(
            remote(column.at[c, at], sums_in.at[c, k], s_send, s_recv.at[c], column_dev(near))
            for k, at in enumerate((near, last))
        )

    def sum_relay(c):
        return remote(sums_in.at[c, 3], sums_in.at[c, 2], s_send, s_far.at[c], column_dev(far))

    def arrived(ref, sem):
        remote(ref, ref, sem, sem, ahead.scatter_of(1)[1]).wait_recv()

    def sent(ref, sem):
        remote(ref, ref, sem, sem, ahead.scatter_of(1)[1]).wait_send()

    for i in range(1, planes):
        notes_copy(ahead, i, n_send, n_recv).start()

    def send_x(way, c):
        for i in range(1, planes):
            x_copy(way, c, i).start()
        column[c, way.gather_at] = x_ref[:, cut(c)]

    def send_ahead(c, carry):
        if flipped:
            for copy in x_first(c):
                copy.start()
            column[c, p] = x_ref[:, cut(c)]
        else:
            send_x(ahead, c)
        return carry

    def relay_x(c):
        arrived(column.at[c, pl.ds(0, 1)], x_far.at[c])
        x_relay(c).start()

    if flipped:
        for i in range(1, QUADS):
            notes_copy(aside, i, f_send, f_recv).start()
        for c in range(straight, chunks):
            send_x(aside, c)
    lax.fori_loop(0, min(2, straight) if flipped else straight, send_ahead, 0)

    load_down.start()
    arrived(notes.at[pl.ds(0, planes - 1)], n_recv)

    earlier = tri(128, tok_mb)

    def spread(way, part):
        pieces = [way.notes[at, m, part] for at in range(planes) for m in range(micro_count)]
        lanes = []
        for at in range(0, len(pieces), 128 // tok_mb):
            block = pieces[at]
            for k, piece in enumerate(pieces[at + 1 : at + 128 // tok_mb]):
                block += pltpu.roll(piece, (k + 1) * tok_mb, 1)
            lanes.append(block)
        return jnp.concatenate(lanes, axis=1)

    def prepare(way, expert):
        ids, weights = spread(way, 0), spread(way, 1)
        named = jnp.zeros((PLANE, depth), jnp.float32)
        share = jnp.zeros((PLANE, depth), jnp.float32)
        for k in range(chosen):
            same = jnp.broadcast_to(ids[k : k + 1], (PLANE, depth)) == expert
            named += jnp.where(same, 1.0, 0.0)
            share += jnp.where(same, jnp.broadcast_to(weights[k : k + 1], (PLANE, depth)), 0.0)
        rank = jnp.concatenate(
            [
                jnp.dot(
                    named[:, at : at + 128].astype(jnp.bfloat16),
                    earlier,
                    preferred_element_type=jnp.float32,
                )
                for at in range(0, depth, 128)
            ],
            axis=1,
        )
        start = lax.div(lax.broadcasted_iota(jnp.int32, (PLANE, depth), 1), tok_mb) * capacity
        spot = jnp.where(named > 0.5, start.astype(jnp.float32) + rank, -1.0)
        place = lax.broadcasted_iota(jnp.int32, (spots, depth), 0).astype(jnp.float32)
        for j in range(PLANE):
            found = place == jnp.broadcast_to(spot[j : j + 1], (spots, depth))
            way.picks[j] = jnp.where(found, 1.0, 0.0).astype(jnp.bfloat16)
        return spot, share

    def weigh(way, spot, share):
        both = jnp.concatenate(
            [spot, share, jnp.zeros((128 - 2 * PLANE, depth), jnp.float32)], axis=0
        ).T
        lane = lax.broadcasted_iota(jnp.int32, (depth, 128), 1).astype(jnp.float32)
        for j in range(PLANE):
            found = lane == jnp.broadcast_to(both[:, j : j + 1], (depth, 128))
            held = jnp.broadcast_to(both[:, PLANE + j : PLANE + j + 1], (depth, 128))
            held = jnp.where(found, held, 0.0)
            high = held.astype(jnp.bfloat16)
            way.shares[j, 0] = high[:, :spots]
            way.shares[j, 1] = (held - high.astype(jnp.float32)).astype(jnp.bfloat16)[:, :spots]

    index = lax.broadcasted_iota(jnp.int32, (PLANE, depth), 0)
    spot, share = prepare(ahead, (p * PLANE + index).astype(jnp.float32))
    for j in range(PLANE):
        own = jnp.sum(share[j : j + 1], axis=1, keepdims=True)
        loads[j] = jnp.broadcast_to(own, loads.shape[1:])
    for i in range(1, PLANE):
        loads_copy(i).start()

    def dispatch(way, c):
        count = planes - 2 if flipped and way is ahead else planes - 1
        arrived(column.at[c, pl.ds(0, count)], x_recv.at[c])
        tokens_here = column[c].reshape(depth, width)
        found = jnp.dot(
            way.picks[...].reshape(PLANE * spots, depth),
            tokens_here,
            preferred_element_type=jnp.float32,
        )
        packed[c] = found.reshape(packed.shape[1:]).astype(jnp.bfloat16)
        for i in range(1, PLANE):
            rows_copy(way, c, i).start()
        rows[c, way.scatter_at] = packed[c, way.scatter_at]

    def reorder(values):
        return jnp.dot(perm[...], values, preferred_element_type=jnp.float32).astype(jnp.bfloat16)

    def consume(way, c):
        for copy in load_in(c):
            copy.wait()
        arrived(rows.at[c, pl.ds(0, PLANE - 1)], d_recv.at[c])
        slot = c % SLOTS
        got = rows[c].reshape(PLANE * spots, width)
        if way is aside:
            got = reorder(got)
        acc_gate[...] += jnp.dot(got, w_gate[slot], preferred_element_type=jnp.float32)
        acc_up[...] += jnp.dot(got, w_up[slot], preferred_element_type=jnp.float32)

        @pl.when(c + SLOTS < chunks)
        def _():
            for copy in load_in(c + SLOTS):
                copy.start()

    def relay_and_send(c):
        relay_x(c)

        @pl.when(c + 2 < straight)
        def _():
            send_ahead(c + 2, 0)

    def step(c, carry):
        pl.when(c < straight)(lambda: dispatch(ahead, c))
        if flipped:
            pl.when(c + AHEAD < straight)(lambda: relay_and_send(c + AHEAD))
            for k in range(flipped):
                pl.when(c == ASIDE[k])(lambda k=k: dispatch(aside, straight + k))
        pl.when(c >= LAG)(lambda: consume(ahead, c - LAG))
        return carry

    if flipped:
        for c in range(AHEAD):
            relay_x(c)
            send_ahead(c + 2, 0)
    lax.fori_loop(0, LAG, step, 0)

    acc_gate[...] = jnp.zeros(acc_gate.shape, jnp.float32)
    acc_up[...] = jnp.zeros(acc_up.shape, jnp.float32)
    if flipped:
        arrived(notes_f.at[pl.ds(0, QUADS - 1)], f_recv)
        expert = lax.div(index, 2) * PLANE + quad * 2 + lax.rem(index, 2)
        spot_f, share_f = prepare(aside, expert.astype(jnp.float32))
        weigh(aside, spot_f, share_f)
        size = perm.shape[0]
        held = spots // planes
        row = lax.broadcasted_iota(jnp.int32, (size, 128), 0)
        group = lax.div(row, held)
        at_plane, at_core, at_quad = lax.rem(group, planes), lax.rem(lax.div(group, planes), 2), lax.div(group, 2 * planes)
        target = (at_plane * PLANE + at_core * QUADS + at_quad) * held + lax.rem(row, held)
        for at in range(0, size, 128):
            lane = at + lax.broadcasted_iota(jnp.int32, (size, 128), 1)
            block = jnp.where(lane == target, 1.0, 0.0).astype(jnp.bfloat16)
            perm[:, at : min(at + 128, size)] = block[:, : min(128, size - at)]
    weigh(ahead, spot, share)

    lax.fori_loop(LAG, straight + LAG, step, 0)
    for c in range(straight, chunks):
        consume(aside, c)

    gate = acc_gate[...]
    hid[...] = (gate / (1.0 + jnp.exp(-gate)) * acc_up[...]).astype(jnp.bfloat16)

    load_down.wait()

    def compute(way, c):
        sent(packed.at[c, pl.ds(0, PLANE - 1)], d_send.at[c])
        found = jnp.dot(hid[...], w_down[:, cut(c)], preferred_element_type=jnp.float32)
        if way is aside:
            found = jnp.dot(
                perm[...], found.astype(jnp.bfloat16), preferred_element_type=jnp.float32
            )
        packed[c] = found.reshape(packed.shape[1:]).astype(jnp.bfloat16)
        for i in range(1, PLANE):
            answer_copy(way, c, i).start()
        inbox[c, way.scatter_at] = packed[c, way.scatter_at]

    def compute_ahead(c, carry):
        compute(ahead, c)
        return carry

    first = min(2, straight)
    lax.fori_loop(0, first, compute_ahead, 0)
    for c in range(straight, chunks):
        compute(aside, c)
    lax.fori_loop(first, straight, compute_ahead, 0)

    arrived(loads_in.at[pl.ds(0, PLANE - 1)], l_recv)
    loads_in[q] = loads[q]
    load_ref[...] = (jnp.sum(loads_in[...], axis=0) * load_scale)[:1, :1]

    def combine(way, c):
        arrived(inbox.at[c, pl.ds(0, PLANE - 1)], a_recv.at[c])
        total = jnp.zeros((depth, width), jnp.float32)
        for k in range(PLANE):
            for half in range(2):
                total += jnp.dot(
                    way.shares[k, half], inbox[c, k], preferred_element_type=jnp.float32
                )
        column[c] = total.reshape(column.shape[1:]).astype(jnp.bfloat16)
        if flipped and way is ahead:
            for copy in sum_first(c):
                copy.start()
        else:
            for i in range(1, planes):
                sum_copy(way, c, i).start()
            sums_in[c, way.gather_at] = column[c, way.gather_at]

    def join(c):
        arrived(sums_in.at[c, pl.ds(0, 2)], s_recv.at[c])
        pair = column[c, far].astype(jnp.float32) + sums_in[c, 1].astype(jnp.float32)
        sums_in[c, 3] = pair.astype(jnp.bfloat16)
        sum_relay(c).start()

    def combine_ahead(c, carry):
        combine(ahead, c)
        if flipped:
            pl.when(c >= 1)(lambda: join(c - 1))
        return carry

    sent(column.at[:, pl.ds(0, planes - 1)], x_send)
    half = straight // 2
    lax.fori_loop(0, half, combine_ahead, 0)
    for c in range(straight, chunks):
        combine(aside, c)
    lax.fori_loop(half, straight, combine_ahead, 0)
    if flipped:
        join(straight - 1)

    def total_joined(c, carry):
        arrived(sums_in.at[c, pl.ds(0, 1)], s_far.at[c])
        total = column[c, p].astype(jnp.float32) + sums_in[c, 0].astype(jnp.float32)
        total += sums_in[c, 2].astype(jnp.float32)
        out_ref[:, cut(c)] = total.astype(jnp.bfloat16)
        return carry

    def gather_sums(c, carry):
        arrived(sums_in.at[c, pl.ds(0, planes - 1)], s_recv.at[c])
        total = sums_in[c, 0].astype(jnp.float32)
        for k in range(1, planes):
            total += sums_in[c, k].astype(jnp.float32)
        out_ref[:, cut(c)] = total.astype(jnp.bfloat16)
        return carry

    lax.fori_loop(0, straight - 1 if flipped else straight, total_joined if flipped else gather_sums, 0)
    lax.fori_loop(straight, chunks, gather_sums, 0)
    if flipped:
        total_joined(straight - 1, 0)

    sent(notes.at[pl.ds(0, planes - 1)], n_send)
    if flipped:
        sent(notes_f.at[pl.ds(0, QUADS - 1)], f_send)
    sent(loads.at[pl.ds(0, PLANE - 1)], l_send)
    sent(column.at[:, pl.ds(0, planes - 1)], s_send)
    sent(packed.at[:, pl.ds(0, PLANE - 1)], a_send)


def layer(x, ids, scores, gate, up, down, devices, tok_mb, capacity, load_scale):
    planes = devices // PLANE
    tokens, model_width = x.shape
    inner = gate.shape[1]
    width = next(w for w in (256, 128) if model_width % w == 0)
    chunks = model_width // width
    spots = planes * (tokens // tok_mb) * capacity
    flipped = FLIPPED if planes == QUADS else 0
    few = (lambda *shape: shape) if flipped else (lambda *shape: (1,) * len(shape))
    dma = pltpu.SemaphoreType.DMA
    vmem = pl.BlockSpec(memory_space=pltpu.VMEM)
    hbm = pl.BlockSpec(memory_space=pl.ANY)
    bf16, f32 = jnp.bfloat16, jnp.float32
    return pl.pallas_call(
        functools.partial(layer_kernel, planes, capacity, tok_mb, load_scale, flipped),
        out_shape=(
            jax.ShapeDtypeStruct((tokens, model_width), bf16),
            jax.ShapeDtypeStruct((1, 1), f32),
        ),
        in_specs=[hbm, vmem, vmem, hbm, hbm, hbm],
        out_specs=(vmem, vmem),
        scratch_shapes=[
            pltpu.VMEM((tokens, model_width), bf16),
            pltpu.VMEM((planes, tokens // tok_mb, 2, ids.shape[1], 128), f32),
            pltpu.VMEM((chunks, planes, tokens, width), bf16),
            pltpu.VMEM((PLANE, spots, planes * tokens), bf16),
            pltpu.VMEM((PLANE, 2, planes * tokens, spots), bf16),
            pltpu.VMEM(few(planes, tokens // tok_mb, 2, ids.shape[1], 128), f32),
            pltpu.VMEM(few(PLANE, spots, planes * tokens), bf16),
            pltpu.VMEM(few(PLANE, 2, planes * tokens, spots), bf16),
            pltpu.VMEM(few(PLANE * spots, PLANE * spots), bf16),
            pltpu.VMEM((chunks, PLANE, spots, width), bf16),
            pltpu.VMEM((chunks, PLANE, spots, width), bf16),
            pltpu.VMEM((PLANE, 8, 128), f32),
            pltpu.VMEM((PLANE, 8, 128), f32),
            pltpu.VMEM((SLOTS, width, inner), bf16),
            pltpu.VMEM((SLOTS, width, inner), bf16),
            pltpu.VMEM((inner, model_width), bf16),
            pltpu.VMEM((PLANE * spots, inner), f32),
            pltpu.VMEM((PLANE * spots, inner), f32),
            pltpu.VMEM((PLANE * spots, inner), bf16),
            pltpu.VMEM((chunks, PLANE, spots, width), bf16),
            pltpu.VMEM((chunks, planes, tokens, width), bf16),
            dma,
            dma((SLOTS,)),
            dma((SLOTS,)),
            dma,
            dma,
            dma,
            dma,
            dma,
            dma((chunks,)),
            dma((chunks,)),
            dma,
            dma((chunks,)),
            dma,
            dma,
            dma((chunks,)),
            dma((chunks,)),
            dma,
            dma((chunks,)),
            dma,
            dma((chunks,)),
        ],
        compiler_params=pltpu.CompilerParams(
            collective_id=0, has_side_effects=True, vmem_limit_bytes=66 * 1000 * 1000
        ),
    )(x, ids, scores, gate, up, down)


def shards(hidden, expert_ids, gate_scores, w_gate, w_up, w_down):
    devices = lax.axis_size("ep")
    micro_count, tok_mb, model_width = hidden.shape
    chosen = expert_ids.shape[2]
    capacity = tok_mb * chosen // devices + 1
    tokens = micro_count * tok_mb
    mixed, expert_load = layer(
        hidden.reshape(tokens, model_width),
        expert_ids.transpose(0, 2, 1),
        gate_scores.transpose(0, 2, 1),
        w_gate[0],
        w_up[0],
        w_down[0],
        devices,
        tok_mb,
        capacity,
        devices / (route_scale * tokens * devices),
    )
    return (mixed.reshape(micro_count, tok_mb, model_width), expert_load.reshape(1))


def solution(mesh):
    placed = (
        P(None, "ep", None),
        P(None, "ep", None),
        P(None, "ep", None),
        P("ep", None, None),
        P("ep", None, None),
        P("ep", None, None),
    )
    return jax.shard_map(
        shards,
        mesh=mesh,
        in_specs=placed,
        out_specs=(P(None, "ep", None), P("ep")),
        check_vma=False,
    )
```

```python
import functools

import jax
import jax.numpy as jnp
from jax import lax
from jax.experimental import pallas as pl
from jax.experimental.pallas import tpu as pltpu
from jax.sharding import PartitionSpec as P

route_scale = 2.5
PLANE = 8
SLOTS = 3
LAG = 4
AHEAD = 2
ASIDE = (5, 8)
FIRST = 1
MIDDLE = 6
QUADS = PLANE // 2
FLIPPED = 2
MESH = pl.DeviceIdType.MESH


class Route:
    def __init__(self, gather_at, gather_of, scatter_at, scatter_of, notes, picks, shares):
        self.gather_at, self.gather_of = gather_at, gather_of
        self.scatter_at, self.scatter_of = scatter_at, scatter_of
        self.notes, self.picks, self.shares = notes, picks, shares


def tri(size, block):
    row = lax.broadcasted_iota(jnp.int32, (size, size), 0)
    col = lax.broadcasted_iota(jnp.int32, (size, size), 1)
    earlier = (row < col) & (lax.div(row, block) == lax.div(col, block))
    return jnp.where(earlier, 1.0, 0.0).astype(jnp.bfloat16)


def layer_kernel(
    planes,
    capacity,
    tok_mb,
    load_scale,
    flipped,
    hidden_ref,
    ids_ref,
    scores_ref,
    gate_ref,
    up_ref,
    down_ref,
    out_ref,
    load_ref,
    x_ref,
    notes,
    column,
    picks,
    shares,
    notes_f,
    picks_f,
    shares_f,
    perm,
    packed,
    rows,
    loads,
    loads_in,
    w_gate,
    w_up,
    w_down,
    acc_gate,
    acc_up,
    hid,
    inbox,
    sums_in,
    hidden_sem,
    gate_sem,
    up_sem,
    down_sem,
    n_send,
    n_recv,
    f_send,
    f_recv,
    x_far,
    s_far,
    x_send,
    x_recv,
    l_send,
    l_recv,
    d_send,
    d_recv,
    a_send,
    a_recv,
    s_send,
    s_recv,
):
    me = lax.axis_index("ep")
    p = me // PLANE
    q = me % PLANE
    quad, core = q // 2, q % 2
    chunks, _, tokens, width = column.shape
    micro_count, chosen, _ = ids_ref.shape
    spots = packed.shape[2]
    depth = planes * tokens
    turned = tuple(chunks - 2 * flipped + 2 * k for k in range(flipped))

    def is_turned(c):
        hit = c == turned[0]
        for at in turned[1:]:
            hit = hit | (c == at)
        return hit

    def is_straight(c):
        good = (c >= 0) & (c < chunks)
        for at in turned:
            good = good & (c != at)
        return good

    def cut(c):
        return pl.ds(pl.multiple_of(c * width, width), width)

    def load_in(c):
        slot = c % SLOTS
        return (
            pltpu.make_async_copy(gate_ref.at[cut(c), :], w_gate.at[slot], gate_sem.at[slot]),
            pltpu.make_async_copy(up_ref.at[cut(c), :], w_up.at[slot], up_sem.at[slot]),
        )

    load_down = pltpu.make_async_copy(down_ref, w_down, down_sem)

    hidden_copy = pltpu.make_async_copy(hidden_ref, x_ref, hidden_sem)
    hidden_copy.start()

    def is_joined(c):
        return is_straight(c) & (c < chunks - 1)

    turn = p * 2 + core
    ahead = Route(
        p,
        lambda i: ((p + i) % planes, ((p + i) % planes) * PLANE + q),
        q,
        lambda i: ((q + i) % PLANE, p * PLANE + (q + i) % PLANE),
        notes,
        picks,
        shares,
    )
    aside = Route(
        quad,
        lambda i: ((quad + i) % QUADS, p * PLANE + ((quad + i) % QUADS) * 2 + core),
        turn,
        lambda i: (
            (turn + i) % (2 * planes),
            ((turn + i) % (2 * planes)) // 2 * PLANE + quad * 2 + (turn + i) % 2,
        ),
        notes_f,
        picks_f,
        shares_f,
    )

    near = p + 1 - 2 * (p % 2)
    far = (p + 2) % planes
    last = (near + 2) % planes

    barrier = pltpu.get_barrier_semaphore()

    def greet(other):
        pl.semaphore_signal(barrier, inc=1, device_id=(other,), device_id_type=MESH)

    for i in range(1, PLANE):
        greet(ahead.scatter_of(i)[1])
    for i in range(1, planes):
        greet(ahead.gather_of(i)[1])
    if flipped:
        for i in range(1, planes):
            greet(((p + i) % planes) * PLANE + quad * 2 + 1 - core)

    for c in range(SLOTS):
        for copy in load_in(c):
            copy.start()

    notes[p] = jnp.zeros(notes.shape[1:], jnp.float32)
    for m in range(micro_count):
        scores = scores_ref[m]
        notes[p, m, 0, :, :tok_mb] = ids_ref[m].astype(jnp.float32)
        notes[p, m, 1, :, :tok_mb] = route_scale * scores / jnp.sum(scores, axis=0, keepdims=True)
    if flipped:
        notes_f[quad] = notes[p]
    hidden_copy.wait()

    pl.semaphore_wait(barrier, PLANE + planes - 2 + (planes - 1 if flipped else 0))

    def remote(src, dst, send, recv, other):
        return pltpu.make_async_remote_copy(
            src_ref=src,
            dst_ref=dst,
            send_sem=send,
            recv_sem=recv,
            device_id=(other,),
            device_id_type=MESH,
        )

    def notes_copy(way, i, send, recv):
        mine = way.notes.at[way.gather_at]
        return remote(mine, mine, send, recv, way.gather_of(i)[1])

    def x_copy(way, c, i):
        place = column.at[c, way.gather_at]
        return remote(x_ref.at[:, cut(c)], place, x_send, x_recv.at[c], way.gather_of(i)[1])

    def loads_copy(i):
        at, other = ahead.scatter_of(i)
        return remote(loads.at[at], loads_in.at[q], l_send, l_recv, other)

    def rows_copy(way, c, i):
        at, other = way.scatter_of(i)
        place = rows.at[c, way.scatter_at]
        return remote(packed.at[c, at], place, d_send.at[c], d_recv.at[c], other)

    def answer_copy(way, c, i):
        at, other = way.scatter_of(i)
        place = inbox.at[c, way.scatter_at]
        return remote(packed.at[c, at], place, a_send, a_recv.at[c], other)

    def sum_copy(way, c, i):
        at, other = way.gather_of(i)
        place = sums_in.at[c, way.gather_at]
        return remote(column.at[c, at], place, s_send, s_recv.at[c], other)

    def column_dev(at):
        return at * PLANE + q

    def x_first(c):
        place = column.at[c, p]
        mine = x_ref.at[:, cut(c)]
        return (
            remote(mine, place, x_send, x_recv.at[c], column_dev(near)),
            remote(mine, place, x_send, x_far.at[c], column_dev(far)),
        )

    def x_relay(c):
        place = column.at[c, far]
        return remote(place, place, x_send, x_recv.at[c], column_dev(near))

    def sum_first(c):
        return tuple(
            remote(column.at[c, at], sums_in.at[c, k], s_send, s_recv.at[c], column_dev(near))
            for k, at in enumerate((near, last))
        )

    def sum_relay(c):
        return remote(sums_in.at[c, 3], sums_in.at[c, 2], s_send, s_far.at[c], column_dev(far))

    def arrived(ref, sem):
        remote(ref, ref, sem, sem, ahead.scatter_of(1)[1]).wait_recv()

    def sent(ref, sem):
        remote(ref, ref, sem, sem, ahead.scatter_of(1)[1]).wait_send()

    for i in range(1, planes):
        notes_copy(ahead, i, n_send, n_recv).start()

    def send_x(way, c):
        for i in range(1, planes):
            x_copy(way, c, i).start()
        column[c, way.gather_at] = x_ref[:, cut(c)]

    def send_ahead(c, carry):
        if flipped:
            for copy in x_first(c):
                copy.start()
            column[c, p] = x_ref[:, cut(c)]
        else:
            send_x(ahead, c)
        return carry

    def relay_x(c):
        arrived(column.at[c, pl.ds(0, 1)], x_far.at[c])
        x_relay(c).start()

    if flipped:
        for i in range(1, QUADS):
            notes_copy(aside, i, f_send, f_recv).start()
        for c in turned:
            send_x(aside, c)
    lax.fori_loop(0, 2 if flipped else chunks, send_ahead, 0)

    load_down.start()
    arrived(notes.at[pl.ds(0, planes - 1)], n_recv)

    earlier = tri(128, tok_mb)

    def spread(way, part):
        pieces = [way.notes[at, m, part] for at in range(planes) for m in range(micro_count)]
        lanes = []
        for at in range(0, len(pieces), 128 // tok_mb):
            block = pieces[at]
            for k, piece in enumerate(pieces[at + 1 : at + 128 // tok_mb]):
                block += pltpu.roll(piece, (k + 1) * tok_mb, 1)
            lanes.append(block)
        return jnp.concatenate(lanes, axis=1)

    def prepare(way, expert):
        ids, weights = spread(way, 0), spread(way, 1)
        named = jnp.zeros((PLANE, depth), jnp.float32)
        share = jnp.zeros((PLANE, depth), jnp.float32)
        for k in range(chosen):
            same = jnp.broadcast_to(ids[k : k + 1], (PLANE, depth)) == expert
            named += jnp.where(same, 1.0, 0.0)
            share += jnp.where(same, jnp.broadcast_to(weights[k : k + 1], (PLANE, depth)), 0.0)
        rank = jnp.concatenate(
            [
                jnp.dot(
                    named[:, at : at + 128].astype(jnp.bfloat16),
                    earlier,
                    preferred_element_type=jnp.float32,
                )
                for at in range(0, depth, 128)
            ],
            axis=1,
        )
        start = lax.div(lax.broadcasted_iota(jnp.int32, (PLANE, depth), 1), tok_mb) * capacity
        spot = jnp.where(named > 0.5, start.astype(jnp.float32) + rank, -1.0)
        place = lax.broadcasted_iota(jnp.int32, (spots, depth), 0).astype(jnp.float32)
        for j in range(PLANE):
            found = place == jnp.broadcast_to(spot[j : j + 1], (spots, depth))
            way.picks[j] = jnp.where(found, 1.0, 0.0).astype(jnp.bfloat16)
        return spot, share

    def weigh(way, spot, share):
        both = jnp.concatenate(
            [spot, share, jnp.zeros((128 - 2 * PLANE, depth), jnp.float32)], axis=0
        ).T
        lane = lax.broadcasted_iota(jnp.int32, (depth, 128), 1).astype(jnp.float32)
        for j in range(PLANE):
            found = lane == jnp.broadcast_to(both[:, j : j + 1], (depth, 128))
            held = jnp.broadcast_to(both[:, PLANE + j : PLANE + j + 1], (depth, 128))
            held = jnp.where(found, held, 0.0)
            high = held.astype(jnp.bfloat16)
            way.shares[j, 0] = high[:, :spots]
            way.shares[j, 1] = (held - high.astype(jnp.float32)).astype(jnp.bfloat16)[:, :spots]

    index = lax.broadcasted_iota(jnp.int32, (PLANE, depth), 0)
    spot, share = prepare(ahead, (p * PLANE + index).astype(jnp.float32))
    for j in range(PLANE):
        own = jnp.sum(share[j : j + 1], axis=1, keepdims=True)
        loads[j] = jnp.broadcast_to(own, loads.shape[1:])
    for i in range(1, PLANE):
        loads_copy(i).start()

    def dispatch(way, c):
        count = planes - 2 if flipped and way is ahead else planes - 1
        arrived(column.at[c, pl.ds(0, count)], x_recv.at[c])
        tokens_here = column[c].reshape(depth, width)
        found = jnp.dot(
            way.picks[...].reshape(PLANE * spots, depth),
            tokens_here,
            preferred_element_type=jnp.float32,
        )
        packed[c] = found.reshape(packed.shape[1:]).astype(jnp.bfloat16)
        for i in range(1, PLANE):
            rows_copy(way, c, i).start()
        rows[c, way.scatter_at] = packed[c, way.scatter_at]

    def reorder(values):
        return jnp.dot(perm[...], values, preferred_element_type=jnp.float32).astype(jnp.bfloat16)

    def consume(way, c, final=False):
        for copy in load_in(c):
            copy.wait()
        arrived(rows.at[c, pl.ds(0, PLANE - 1)], d_recv.at[c])
        slot = c % SLOTS
        got = rows[c].reshape(PLANE * spots, width)
        if way is aside:
            got = reorder(got)
        if final:
            for at in range(0, hid.shape[1], 256):
                tile = slice(at, at + 256)
                gate = acc_gate[:, tile] + jnp.dot(
                    got, w_gate[slot, :, tile], preferred_element_type=jnp.float32
                )
                upper = acc_up[:, tile] + jnp.dot(
                    got, w_up[slot, :, tile], preferred_element_type=jnp.float32
                )
                hid[:, tile] = (gate / (1.0 + jnp.exp(-gate)) * upper).astype(jnp.bfloat16)
            return
        acc_gate[...] += jnp.dot(got, w_gate[slot], preferred_element_type=jnp.float32)
        acc_up[...] += jnp.dot(got, w_up[slot], preferred_element_type=jnp.float32)

        @pl.when(c + SLOTS < chunks)
        def _():
            for copy in load_in(c + SLOTS):
                copy.start()

    def step(c, carry):
        pl.when(is_straight(c))(lambda: dispatch(ahead, c))
        if flipped:
            pl.when(is_straight(c + AHEAD))(lambda: relay_x(c + AHEAD))

            @pl.when(is_straight(c + AHEAD + 2))
            def _():
                send_ahead(c + AHEAD + 2, 0)

            for k in range(flipped):
                pl.when(c == ASIDE[k])(lambda k=k: dispatch(aside, turned[k]))
            pl.when(is_turned(c - LAG))(lambda: consume(aside, c - LAG))
        pl.when(is_straight(c - LAG))(lambda: consume(ahead, c - LAG))
        return carry

    if flipped:
        for c in range(AHEAD):
            relay_x(c)
            send_ahead(c + 2, 0)
    lax.fori_loop(0, LAG, step, 0)

    acc_gate[...] = jnp.zeros(acc_gate.shape, jnp.float32)
    acc_up[...] = jnp.zeros(acc_up.shape, jnp.float32)
    if flipped:
        arrived(notes_f.at[pl.ds(0, QUADS - 1)], f_recv)
        expert = lax.div(index, 2) * PLANE + quad * 2 + lax.rem(index, 2)
        spot_f, share_f = prepare(aside, expert.astype(jnp.float32))
        weigh(aside, spot_f, share_f)
        size = perm.shape[0]
        held = spots // planes
        row = lax.broadcasted_iota(jnp.int32, (size, 128), 0)
        group = lax.div(row, held)
        at_plane, at_core, at_quad = lax.rem(group, planes), lax.rem(lax.div(group, planes), 2), lax.div(group, 2 * planes)
        target = (at_plane * PLANE + at_core * QUADS + at_quad) * held + lax.rem(row, held)
        for at in range(0, size, 128):
            lane = at + lax.broadcasted_iota(jnp.int32, (size, 128), 1)
            block = jnp.where(lane == target, 1.0, 0.0).astype(jnp.bfloat16)
            perm[:, at : min(at + 128, size)] = block[:, : min(128, size - at)]
    weigh(ahead, spot, share)

    lax.fori_loop(LAG, chunks + LAG - 1, step, 0)
    consume(ahead, chunks - 1, True)


    load_down.wait()

    def compute(way, c):
        sent(packed.at[c, pl.ds(0, PLANE - 1)], d_send.at[c])
        found = jnp.dot(hid[...], w_down[:, cut(c)], preferred_element_type=jnp.float32)
        if way is aside:
            found = jnp.dot(
                perm[...], found.astype(jnp.bfloat16), preferred_element_type=jnp.float32
            )
        packed[c] = found.reshape(packed.shape[1:]).astype(jnp.bfloat16)
        for i in range(1, PLANE):
            answer_copy(way, c, i).start()
        inbox[c, way.scatter_at] = packed[c, way.scatter_at]

    def compute_ahead(c, carry):
        pl.when(is_straight(c))(lambda: compute(ahead, c))
        for k in range(flipped):
            pl.when(c == FIRST + k)(lambda k=k: compute(aside, turned[k]))
        return carry

    lax.fori_loop(0, chunks, compute_ahead, 0)

    arrived(loads_in.at[pl.ds(0, PLANE - 1)], l_recv)
    loads_in[q] = loads[q]
    load_ref[...] = (jnp.sum(loads_in[...], axis=0) * load_scale)[:1, :1]

    def combine(way, c, joined=False):
        arrived(inbox.at[c, pl.ds(0, PLANE - 1)], a_recv.at[c])
        total = jnp.zeros((depth, width), jnp.float32)
        for k in range(PLANE):
            for half in range(2):
                total += jnp.dot(
                    way.shares[k, half], inbox[c, k], preferred_element_type=jnp.float32
                )
        column[c] = total.reshape(column.shape[1:]).astype(jnp.bfloat16)
        if joined:
            for copy in sum_first(c):
                copy.start()
        else:
            for i in range(1, planes):
                sum_copy(way, c, i).start()
            sums_in[c, way.gather_at] = column[c, way.gather_at]

    def join(c):
        arrived(sums_in.at[c, pl.ds(0, 2)], s_recv.at[c])
        pair = column[c, far].astype(jnp.float32) + sums_in[c, 1].astype(jnp.float32)
        sums_in[c, 3] = pair.astype(jnp.bfloat16)
        sum_relay(c).start()

    def combine_ahead(c, carry):
        if flipped:
            pl.when(is_joined(c))(lambda: combine(ahead, c, True))
            pl.when(c == chunks - 1)(lambda: combine(ahead, c))
            pl.when(is_joined(c - 1))(lambda: join(c - 1))
            for k in range(flipped):
                pl.when(c == MIDDLE + k)(lambda k=k: combine(aside, turned[k]))
        else:
            combine(ahead, c)
        return carry

    sent(column.at[:, pl.ds(0, planes - 1)], x_send)
    lax.fori_loop(0, chunks, combine_ahead, 0)

    def total_joined(c):
        arrived(sums_in.at[c, pl.ds(0, 1)], s_far.at[c])
        total = column[c, p].astype(jnp.float32) + sums_in[c, 0].astype(jnp.float32)
        total += sums_in[c, 2].astype(jnp.float32)
        out_ref[:, cut(c)] = total.astype(jnp.bfloat16)

    def gather_sums(c):
        arrived(sums_in.at[c, pl.ds(0, planes - 1)], s_recv.at[c])
        total = sums_in[c, 0].astype(jnp.float32)
        for k in range(1, planes):
            total += sums_in[c, k].astype(jnp.float32)
        out_ref[:, cut(c)] = total.astype(jnp.bfloat16)

    def finish(c, carry):
        if flipped:
            pl.when(is_turned(c) | (c == chunks - 1))(lambda: gather_sums(c))
            pl.when(is_joined(c))(lambda: total_joined(c))
        else:
            gather_sums(c)
        return carry

    lax.fori_loop(0, chunks, finish, 0)

    sent(notes.at[pl.ds(0, planes - 1)], n_send)
    if flipped:
        sent(notes_f.at[pl.ds(0, QUADS - 1)], f_send)
    sent(loads.at[pl.ds(0, PLANE - 1)], l_send)
    sent(column.at[:, pl.ds(0, planes - 1)], s_send)
    sent(packed.at[:, pl.ds(0, PLANE - 1)], a_send)


def layer(x, ids, scores, gate, up, down, devices, tok_mb, capacity, load_scale):
    planes = devices // PLANE
    tokens, model_width = x.shape
    inner = gate.shape[1]
    width = next(w for w in (256, 128) if model_width % w == 0)
    chunks = model_width // width
    spots = planes * (tokens // tok_mb) * capacity
    flipped = FLIPPED if planes == QUADS else 0
    few = (lambda *shape: shape) if flipped else (lambda *shape: (1,) * len(shape))
    dma = pltpu.SemaphoreType.DMA
    vmem = pl.BlockSpec(memory_space=pltpu.VMEM)
    hbm = pl.BlockSpec(memory_space=pl.ANY)
    bf16, f32 = jnp.bfloat16, jnp.float32
    return pl.pallas_call(
        functools.partial(layer_kernel, planes, capacity, tok_mb, load_scale, flipped),
        out_shape=(
            jax.ShapeDtypeStruct((tokens, model_width), bf16),
            jax.ShapeDtypeStruct((1, 1), f32),
        ),
        in_specs=[hbm, vmem, vmem, hbm, hbm, hbm],
        out_specs=(vmem, vmem),
        scratch_shapes=[
            pltpu.VMEM((tokens, model_width), bf16),
            pltpu.VMEM((planes, tokens // tok_mb, 2, ids.shape[1], 128), f32),
            pltpu.VMEM((chunks, planes, tokens, width), bf16),
            pltpu.VMEM((PLANE, spots, planes * tokens), bf16),
            pltpu.VMEM((PLANE, 2, planes * tokens, spots), bf16),
            pltpu.VMEM(few(planes, tokens // tok_mb, 2, ids.shape[1], 128), f32),
            pltpu.VMEM(few(PLANE, spots, planes * tokens), bf16),
            pltpu.VMEM(few(PLANE, 2, planes * tokens, spots), bf16),
            pltpu.VMEM(few(PLANE * spots, PLANE * spots), bf16),
            pltpu.VMEM((chunks, PLANE, spots, width), bf16),
            pltpu.VMEM((chunks, PLANE, spots, width), bf16),
            pltpu.VMEM((PLANE, 8, 128), f32),
            pltpu.VMEM((PLANE, 8, 128), f32),
            pltpu.VMEM((SLOTS, width, inner), bf16),
            pltpu.VMEM((SLOTS, width, inner), bf16),
            pltpu.VMEM((inner, model_width), bf16),
            pltpu.VMEM((PLANE * spots, inner), f32),
            pltpu.VMEM((PLANE * spots, inner), f32),
            pltpu.VMEM((PLANE * spots, inner), bf16),
            pltpu.VMEM((chunks, PLANE, spots, width), bf16),
            pltpu.VMEM((chunks, planes, tokens, width), bf16),
            dma,
            dma((SLOTS,)),
            dma((SLOTS,)),
            dma,
            dma,
            dma,
            dma,
            dma,
            dma((chunks,)),
            dma((chunks,)),
            dma,
            dma((chunks,)),
            dma,
            dma,
            dma((chunks,)),
            dma((chunks,)),
            dma,
            dma((chunks,)),
            dma,
            dma((chunks,)),
        ],
        compiler_params=pltpu.CompilerParams(
            collective_id=0, has_side_effects=True, vmem_limit_bytes=66 * 1000 * 1000
        ),
    )(x, ids, scores, gate, up, down)


def shards(hidden, expert_ids, gate_scores, w_gate, w_up, w_down):
    devices = lax.axis_size("ep")
    micro_count, tok_mb, model_width = hidden.shape
    chosen = expert_ids.shape[2]
    capacity = tok_mb * chosen // devices + 1
    tokens = micro_count * tok_mb
    mixed, expert_load = layer(
        hidden.reshape(tokens, model_width),
        expert_ids.transpose(0, 2, 1),
        gate_scores.transpose(0, 2, 1),
        w_gate[0],
        w_up[0],
        w_down[0],
        devices,
        tok_mb,
        capacity,
        devices / (route_scale * tokens * devices),
    )
    return (mixed.reshape(micro_count, tok_mb, model_width), expert_load.reshape(1))


def solution(mesh):
    placed = (
        P(None, "ep", None),
        P(None, "ep", None),
        P(None, "ep", None),
        P("ep", None, None),
        P("ep", None, None),
        P("ep", None, None),
    )
    return jax.shard_map(
        shards,
        mesh=mesh,
        in_specs=placed,
        out_specs=(P(None, "ep", None), P("ep")),
        check_vma=False,
    )
```

```python
import functools

import jax
import jax.numpy as jnp
from jax import lax
from jax.experimental import pallas as pl
from jax.experimental.pallas import tpu as pltpu
from jax.sharding import PartitionSpec as P

route_scale = 2.5
PLANE = 8
SLOTS = 3
LAG = 4
AHEAD = 2
ASIDE = (5, 8)
FIRST = 1
MIDDLE = 6
QUADS = PLANE // 2
ORDER = ((1, 1, 0), (1, 1, 1), (0, 1, 0), (1, 0, 0), (0, 1, 1), (1, 0, 1), (0, 0, 1))
FLIPPED = 2
MESH = pl.DeviceIdType.MESH


class Route:
    def __init__(self, gather_at, gather_of, scatter_at, scatter_of, notes, picks, shares):
        self.gather_at, self.gather_of = gather_at, gather_of
        self.scatter_at, self.scatter_of = scatter_at, scatter_of
        self.notes, self.picks, self.shares = notes, picks, shares


def tri(size, block):
    row = lax.broadcasted_iota(jnp.int32, (size, size), 0)
    col = lax.broadcasted_iota(jnp.int32, (size, size), 1)
    earlier = (row < col) & (lax.div(row, block) == lax.div(col, block))
    return jnp.where(earlier, 1.0, 0.0).astype(jnp.bfloat16)


def layer_kernel(
    planes,
    capacity,
    tok_mb,
    load_scale,
    flipped,
    hidden_ref,
    ids_ref,
    scores_ref,
    gate_ref,
    up_ref,
    down_ref,
    out_ref,
    load_ref,
    x_ref,
    notes,
    column,
    picks,
    shares,
    notes_f,
    picks_f,
    shares_f,
    perm,
    packed,
    rows,
    loads,
    loads_in,
    w_gate,
    w_up,
    w_down,
    acc_gate,
    acc_up,
    hid,
    inbox,
    sums_in,
    hidden_sem,
    gate_sem,
    up_sem,
    down_sem,
    n_send,
    n_recv,
    f_send,
    f_recv,
    x_far,
    s_far,
    x_send,
    x_recv,
    l_send,
    l_recv,
    d_send,
    d_recv,
    a_send,
    a_recv,
    s_send,
    s_recv,
):
    me = lax.axis_index("ep")
    p = me // PLANE
    q = me % PLANE
    quad, core = q // 2, q % 2
    chunks, _, tokens, width = column.shape
    micro_count, chosen, _ = ids_ref.shape
    spots = packed.shape[2]
    depth = planes * tokens
    turned = tuple(chunks - 2 * flipped + 2 * k for k in range(flipped))

    def is_turned(c):
        hit = c == turned[0]
        for at in turned[1:]:
            hit = hit | (c == at)
        return hit

    def is_straight(c):
        good = (c >= 0) & (c < chunks)
        for at in turned:
            good = good & (c != at)
        return good

    def cut(c):
        return pl.ds(pl.multiple_of(c * width, width), width)

    def load_in(c):
        slot = c % SLOTS
        return (
            pltpu.make_async_copy(gate_ref.at[cut(c), :], w_gate.at[slot], gate_sem.at[slot]),
            pltpu.make_async_copy(up_ref.at[cut(c), :], w_up.at[slot], up_sem.at[slot]),
        )

    load_down = pltpu.make_async_copy(down_ref, w_down, down_sem)

    hidden_copy = pltpu.make_async_copy(hidden_ref, x_ref, hidden_sem)
    hidden_copy.start()

    def is_joined(c):
        return is_straight(c) & (c < chunks - 1)

    def beside(i):
        y, x, c = ORDER[i - 1]
        at = (q // 4 + y) % 2 * 4 + (quad + x) % 2 * 2 + (core + c) % 2
        return at, p * PLANE + at

    turn = p * 2 + core
    ahead = Route(
        p,
        lambda i: ((p + i) % planes, ((p + i) % planes) * PLANE + q),
        q,
        beside,
        notes,
        picks,
        shares,
    )
    aside = Route(
        quad,
        lambda i: ((quad + i) % QUADS, p * PLANE + ((quad + i) % QUADS) * 2 + core),
        turn,
        lambda i: (
            (turn + i) % (2 * planes),
            ((turn + i) % (2 * planes)) // 2 * PLANE + quad * 2 + (turn + i) % 2,
        ),
        notes_f,
        picks_f,
        shares_f,
    )

    near = p + 1 - 2 * (p % 2)
    far = (p + 2) % planes
    last = (near + 2) % planes

    barrier = pltpu.get_barrier_semaphore()

    def greet(other):
        pl.semaphore_signal(barrier, inc=1, device_id=(other,), device_id_type=MESH)

    for i in range(1, PLANE):
        greet(ahead.scatter_of(i)[1])
    for i in range(1, planes):
        greet(ahead.gather_of(i)[1])
    if flipped:
        for i in range(1, planes):
            greet(((p + i) % planes) * PLANE + quad * 2 + 1 - core)

    for c in range(SLOTS):
        for copy in load_in(c):
            copy.start()

    notes[p] = jnp.zeros(notes.shape[1:], jnp.float32)
    for m in range(micro_count):
        scores = scores_ref[m]
        notes[p, m, 0, :, :tok_mb] = ids_ref[m].astype(jnp.float32)
        notes[p, m, 1, :, :tok_mb] = route_scale * scores / jnp.sum(scores, axis=0, keepdims=True)
    if flipped:
        notes_f[quad] = notes[p]
    hidden_copy.wait()

    pl.semaphore_wait(barrier, PLANE + planes - 2 + (planes - 1 if flipped else 0))

    def remote(src, dst, send, recv, other):
        return pltpu.make_async_remote_copy(
            src_ref=src,
            dst_ref=dst,
            send_sem=send,
            recv_sem=recv,
            device_id=(other,),
            device_id_type=MESH,
        )

    def notes_copy(way, i, send, recv):
        mine = way.notes.at[way.gather_at]
        return remote(mine, mine, send, recv, way.gather_of(i)[1])

    def x_copy(way, c, i):
        place = column.at[c, way.gather_at]
        return remote(x_ref.at[:, cut(c)], place, x_send, x_recv.at[c], way.gather_of(i)[1])

    def loads_copy(i):
        at, other = ahead.scatter_of(i)
        return remote(loads.at[at], loads_in.at[q], l_send, l_recv, other)

    def rows_copy(way, c, i):
        at, other = way.scatter_of(i)
        place = rows.at[c, way.scatter_at]
        return remote(packed.at[c, at], place, d_send.at[c], d_recv.at[c], other)

    def answer_copy(way, c, i):
        at, other = way.scatter_of(i)
        place = inbox.at[c, way.scatter_at]
        return remote(packed.at[c, at], place, a_send, a_recv.at[c], other)

    def sum_copy(way, c, i):
        at, other = way.gather_of(i)
        place = sums_in.at[c, way.gather_at]
        return remote(column.at[c, at], place, s_send, s_recv.at[c], other)

    def column_dev(at):
        return at * PLANE + q

    def x_first(c):
        place = column.at[c, p]
        mine = x_ref.at[:, cut(c)]
        return (
            remote(mine, place, x_send, x_recv.at[c], column_dev(near)),
            remote(mine, place, x_send, x_far.at[c], column_dev(far)),
        )

    def x_relay(c):
        place = column.at[c, far]
        return remote(place, place, x_send, x_recv.at[c], column_dev(near))

    def sum_first(c):
        return tuple(
            remote(column.at[c, at], sums_in.at[c, k], s_send, s_recv.at[c], column_dev(near))
            for k, at in enumerate((near, last))
        )

    def sum_relay(c):
        return remote(sums_in.at[c, 3], sums_in.at[c, 2], s_send, s_far.at[c], column_dev(far))

    def arrived(ref, sem):
        remote(ref, ref, sem, sem, ahead.scatter_of(1)[1]).wait_recv()

    def sent(ref, sem):
        remote(ref, ref, sem, sem, ahead.scatter_of(1)[1]).wait_send()

    for i in range(1, planes):
        notes_copy(ahead, i, n_send, n_recv).start()

    def send_x(way, c):
        for i in range(1, planes):
            x_copy(way, c, i).start()
        column[c, way.gather_at] = x_ref[:, cut(c)]

    def send_ahead(c, carry):
        if flipped:
            for copy in x_first(c):
                copy.start()
            column[c, p] = x_ref[:, cut(c)]
        else:
            send_x(ahead, c)
        return carry

    def relay_x(c):
        arrived(column.at[c, pl.ds(0, 1)], x_far.at[c])
        x_relay(c).start()

    if flipped:
        for i in range(1, QUADS):
            notes_copy(aside, i, f_send, f_recv).start()
        for c in turned:
            send_x(aside, c)
    lax.fori_loop(0, 2 if flipped else chunks, send_ahead, 0)

    load_down.start()
    arrived(notes.at[pl.ds(0, planes - 1)], n_recv)

    earlier = tri(128, tok_mb)

    def spread(way, part):
        pieces = [way.notes[at, m, part] for at in range(planes) for m in range(micro_count)]
        lanes = []
        for at in range(0, len(pieces), 128 // tok_mb):
            block = pieces[at]
            for k, piece in enumerate(pieces[at + 1 : at + 128 // tok_mb]):
                block += pltpu.roll(piece, (k + 1) * tok_mb, 1)
            lanes.append(block)
        return jnp.concatenate(lanes, axis=1)

    def prepare(way, expert):
        ids, weights = spread(way, 0), spread(way, 1)
        named = jnp.zeros((PLANE, depth), jnp.float32)
        share = jnp.zeros((PLANE, depth), jnp.float32)
        for k in range(chosen):
            same = jnp.broadcast_to(ids[k : k + 1], (PLANE, depth)) == expert
            named += jnp.where(same, 1.0, 0.0)
            share += jnp.where(same, jnp.broadcast_to(weights[k : k + 1], (PLANE, depth)), 0.0)
        rank = jnp.concatenate(
            [
                jnp.dot(
                    named[:, at : at + 128].astype(jnp.bfloat16),
                    earlier,
                    preferred_element_type=jnp.float32,
                )
                for at in range(0, depth, 128)
            ],
            axis=1,
        )
        start = lax.div(lax.broadcasted_iota(jnp.int32, (PLANE, depth), 1), tok_mb) * capacity
        spot = jnp.where(named > 0.5, start.astype(jnp.float32) + rank, -1.0)
        place = lax.broadcasted_iota(jnp.int32, (spots, depth), 0).astype(jnp.float32)
        for j in range(PLANE):
            found = place == jnp.broadcast_to(spot[j : j + 1], (spots, depth))
            way.picks[j] = jnp.where(found, 1.0, 0.0).astype(jnp.bfloat16)
        return spot, share

    def weigh(way, spot, share):
        both = jnp.concatenate(
            [spot, share, jnp.zeros((128 - 2 * PLANE, depth), jnp.float32)], axis=0
        ).T
        lane = lax.broadcasted_iota(jnp.int32, (depth, 128), 1).astype(jnp.float32)
        for j in range(PLANE):
            found = lane == jnp.broadcast_to(both[:, j : j + 1], (depth, 128))
            held = jnp.broadcast_to(both[:, PLANE + j : PLANE + j + 1], (depth, 128))
            held = jnp.where(found, held, 0.0)
            high = held.astype(jnp.bfloat16)
            way.shares[j, 0] = high[:, :spots]
            way.shares[j, 1] = (held - high.astype(jnp.float32)).astype(jnp.bfloat16)[:, :spots]

    index = lax.broadcasted_iota(jnp.int32, (PLANE, depth), 0)
    spot, share = prepare(ahead, (p * PLANE + index).astype(jnp.float32))
    for j in range(PLANE):
        own = jnp.sum(share[j : j + 1], axis=1, keepdims=True)
        loads[j] = jnp.broadcast_to(own, loads.shape[1:])
    for i in range(1, PLANE):
        loads_copy(i).start()

    def dispatch(way, c):
        count = planes - 2 if flipped and way is ahead else planes - 1
        arrived(column.at[c, pl.ds(0, count)], x_recv.at[c])
        tokens_here = column[c].reshape(depth, width)
        found = jnp.dot(
            way.picks[...].reshape(PLANE * spots, depth),
            tokens_here,
            preferred_element_type=jnp.float32,
        )
        packed[c] = found.reshape(packed.shape[1:]).astype(jnp.bfloat16)
        for i in range(1, PLANE):
            rows_copy(way, c, i).start()
        rows[c, way.scatter_at] = packed[c, way.scatter_at]

    def reorder(values):
        return jnp.dot(perm[...], values, preferred_element_type=jnp.float32).astype(jnp.bfloat16)

    def consume(way, c, final=False):
        for copy in load_in(c):
            copy.wait()
        arrived(rows.at[c, pl.ds(0, PLANE - 1)], d_recv.at[c])
        slot = c % SLOTS
        got = rows[c].reshape(PLANE * spots, width)
        if way is aside:
            got = reorder(got)
        if final:
            for at in range(0, hid.shape[1], 256):
                tile = slice(at, at + 256)
                gate = acc_gate[:, tile] + jnp.dot(
                    got, w_gate[slot, :, tile], preferred_element_type=jnp.float32
                )
                upper = acc_up[:, tile] + jnp.dot(
                    got, w_up[slot, :, tile], preferred_element_type=jnp.float32
                )
                hid[:, tile] = (gate / (1.0 + jnp.exp(-gate)) * upper).astype(jnp.bfloat16)
            return
        acc_gate[...] += jnp.dot(got, w_gate[slot], preferred_element_type=jnp.float32)
        acc_up[...] += jnp.dot(got, w_up[slot], preferred_element_type=jnp.float32)

        @pl.when(c + SLOTS < chunks)
        def _():
            for copy in load_in(c + SLOTS):
                copy.start()

    def step(c, carry):
        pl.when(is_straight(c))(lambda: dispatch(ahead, c))
        if flipped:
            pl.when(is_straight(c + AHEAD))(lambda: relay_x(c + AHEAD))

            @pl.when(is_straight(c + AHEAD + 2))
            def _():
                send_ahead(c + AHEAD + 2, 0)

            for k in range(flipped):
                pl.when(c == ASIDE[k])(lambda k=k: dispatch(aside, turned[k]))
            pl.when(is_turned(c - LAG))(lambda: consume(aside, c - LAG))
        pl.when(is_straight(c - LAG))(lambda: consume(ahead, c - LAG))
        return carry

    if flipped:
        for c in range(AHEAD):
            relay_x(c)
            send_ahead(c + 2, 0)
    lax.fori_loop(0, LAG, step, 0)

    acc_gate[...] = jnp.zeros(acc_gate.shape, jnp.float32)
    acc_up[...] = jnp.zeros(acc_up.shape, jnp.float32)
    if flipped:
        arrived(notes_f.at[pl.ds(0, QUADS - 1)], f_recv)
        expert = lax.div(index, 2) * PLANE + quad * 2 + lax.rem(index, 2)
        spot_f, share_f = prepare(aside, expert.astype(jnp.float32))
        weigh(aside, spot_f, share_f)
        size = perm.shape[0]
        held = spots // planes
        row = lax.broadcasted_iota(jnp.int32, (size, 128), 0)
        group = lax.div(row, held)
        at_plane, at_core, at_quad = lax.rem(group, planes), lax.rem(lax.div(group, planes), 2), lax.div(group, 2 * planes)
        target = (at_plane * PLANE + at_core * QUADS + at_quad) * held + lax.rem(row, held)
        for at in range(0, size, 128):
            lane = at + lax.broadcasted_iota(jnp.int32, (size, 128), 1)
            block = jnp.where(lane == target, 1.0, 0.0).astype(jnp.bfloat16)
            perm[:, at : min(at + 128, size)] = block[:, : min(128, size - at)]
    weigh(ahead, spot, share)

    lax.fori_loop(LAG, chunks + LAG - 1, step, 0)
    consume(ahead, chunks - 1, True)


    load_down.wait()

    def compute(way, c):
        sent(packed.at[c, pl.ds(0, PLANE - 1)], d_send.at[c])
        found = jnp.dot(hid[...], w_down[:, cut(c)], preferred_element_type=jnp.float32)
        if way is aside:
            found = jnp.dot(
                perm[...], found.astype(jnp.bfloat16), preferred_element_type=jnp.float32
            )
        packed[c] = found.reshape(packed.shape[1:]).astype(jnp.bfloat16)
        for i in range(1, PLANE):
            answer_copy(way, c, i).start()
        inbox[c, way.scatter_at] = packed[c, way.scatter_at]

    def compute_ahead(c, carry):
        pl.when(is_straight(c))(lambda: compute(ahead, c))
        for k in range(flipped):
            pl.when(c == FIRST + k)(lambda k=k: compute(aside, turned[k]))
        return carry

    lax.fori_loop(0, chunks, compute_ahead, 0)

    arrived(loads_in.at[pl.ds(0, PLANE - 1)], l_recv)
    loads_in[q] = loads[q]
    load_ref[...] = (jnp.sum(loads_in[...], axis=0) * load_scale)[:1, :1]

    def combine(way, c, joined=False):
        arrived(inbox.at[c, pl.ds(0, PLANE - 1)], a_recv.at[c])
        total = jnp.zeros((depth, width), jnp.float32)
        for k in range(PLANE):
            for half in range(2):
                total += jnp.dot(
                    way.shares[k, half], inbox[c, k], preferred_element_type=jnp.float32
                )
        column[c] = total.reshape(column.shape[1:]).astype(jnp.bfloat16)
        if joined:
            for copy in sum_first(c):
                copy.start()
        else:
            for i in range(1, planes):
                sum_copy(way, c, i).start()
            sums_in[c, way.gather_at] = column[c, way.gather_at]

    def join(c):
        arrived(sums_in.at[c, pl.ds(0, 2)], s_recv.at[c])
        pair = column[c, far].astype(jnp.float32) + sums_in[c, 1].astype(jnp.float32)
        sums_in[c, 3] = pair.astype(jnp.bfloat16)
        sum_relay(c).start()

    def combine_ahead(c, carry):
        if flipped:
            pl.when(is_joined(c))(lambda: combine(ahead, c, True))
            pl.when(c == chunks - 1)(lambda: combine(ahead, c))
            pl.when(is_joined(c - 1))(lambda: join(c - 1))
            for k in range(flipped):
                pl.when(c == MIDDLE + k)(lambda k=k: combine(aside, turned[k]))
        else:
            combine(ahead, c)
        return carry

    sent(column.at[:, pl.ds(0, planes - 1)], x_send)
    lax.fori_loop(0, chunks, combine_ahead, 0)

    def total_joined(c):
        arrived(sums_in.at[c, pl.ds(0, 1)], s_far.at[c])
        total = column[c, p].astype(jnp.float32) + sums_in[c, 0].astype(jnp.float32)
        total += sums_in[c, 2].astype(jnp.float32)
        out_ref[:, cut(c)] = total.astype(jnp.bfloat16)

    def gather_sums(c):
        arrived(sums_in.at[c, pl.ds(0, planes - 1)], s_recv.at[c])
        total = sums_in[c, 0].astype(jnp.float32)
        for k in range(1, planes):
            total += sums_in[c, k].astype(jnp.float32)
        out_ref[:, cut(c)] = total.astype(jnp.bfloat16)

    def finish(c, carry):
        if flipped:
            pl.when(is_turned(c) | (c == chunks - 1))(lambda: gather_sums(c))
            pl.when(is_joined(c))(lambda: total_joined(c))
        else:
            gather_sums(c)
        return carry

    lax.fori_loop(0, chunks, finish, 0)

    sent(notes.at[pl.ds(0, planes - 1)], n_send)
    if flipped:
        sent(notes_f.at[pl.ds(0, QUADS - 1)], f_send)
    sent(loads.at[pl.ds(0, PLANE - 1)], l_send)
    sent(column.at[:, pl.ds(0, planes - 1)], s_send)
    sent(packed.at[:, pl.ds(0, PLANE - 1)], a_send)


def layer(x, ids, scores, gate, up, down, devices, tok_mb, capacity, load_scale):
    planes = devices // PLANE
    tokens, model_width = x.shape
    inner = gate.shape[1]
    width = next(w for w in (256, 128) if model_width % w == 0)
    chunks = model_width // width
    spots = planes * (tokens // tok_mb) * capacity
    flipped = FLIPPED if planes == QUADS else 0
    few = (lambda *shape: shape) if flipped else (lambda *shape: (1,) * len(shape))
    dma = pltpu.SemaphoreType.DMA
    vmem = pl.BlockSpec(memory_space=pltpu.VMEM)
    hbm = pl.BlockSpec(memory_space=pl.ANY)
    bf16, f32 = jnp.bfloat16, jnp.float32
    return pl.pallas_call(
        functools.partial(layer_kernel, planes, capacity, tok_mb, load_scale, flipped),
        out_shape=(
            jax.ShapeDtypeStruct((tokens, model_width), bf16),
            jax.ShapeDtypeStruct((1, 1), f32),
        ),
        in_specs=[hbm, vmem, vmem, hbm, hbm, hbm],
        out_specs=(vmem, vmem),
        scratch_shapes=[
            pltpu.VMEM((tokens, model_width), bf16),
            pltpu.VMEM((planes, tokens // tok_mb, 2, ids.shape[1], 128), f32),
            pltpu.VMEM((chunks, planes, tokens, width), bf16),
            pltpu.VMEM((PLANE, spots, planes * tokens), bf16),
            pltpu.VMEM((PLANE, 2, planes * tokens, spots), bf16),
            pltpu.VMEM(few(planes, tokens // tok_mb, 2, ids.shape[1], 128), f32),
            pltpu.VMEM(few(PLANE, spots, planes * tokens), bf16),
            pltpu.VMEM(few(PLANE, 2, planes * tokens, spots), bf16),
            pltpu.VMEM(few(PLANE * spots, PLANE * spots), bf16),
            pltpu.VMEM((chunks, PLANE, spots, width), bf16),
            pltpu.VMEM((chunks, PLANE, spots, width), bf16),
            pltpu.VMEM((PLANE, 8, 128), f32),
            pltpu.VMEM((PLANE, 8, 128), f32),
            pltpu.VMEM((SLOTS, width, inner), bf16),
            pltpu.VMEM((SLOTS, width, inner), bf16),
            pltpu.VMEM((inner, model_width), bf16),
            pltpu.VMEM((PLANE * spots, inner), f32),
            pltpu.VMEM((PLANE * spots, inner), f32),
            pltpu.VMEM((PLANE * spots, inner), bf16),
            pltpu.VMEM((chunks, PLANE, spots, width), bf16),
            pltpu.VMEM((chunks, planes, tokens, width), bf16),
            dma,
            dma((SLOTS,)),
            dma((SLOTS,)),
            dma,
            dma,
            dma,
            dma,
            dma,
            dma((chunks,)),
            dma((chunks,)),
            dma,
            dma((chunks,)),
            dma,
            dma,
            dma((chunks,)),
            dma((chunks,)),
            dma,
            dma((chunks,)),
            dma,
            dma((chunks,)),
        ],
        compiler_params=pltpu.CompilerParams(
            collective_id=0, has_side_effects=True, vmem_limit_bytes=66 * 1000 * 1000
        ),
    )(x, ids, scores, gate, up, down)


def shards(hidden, expert_ids, gate_scores, w_gate, w_up, w_down):
    devices = lax.axis_size("ep")
    micro_count, tok_mb, model_width = hidden.shape
    chosen = expert_ids.shape[2]
    capacity = tok_mb * chosen // devices + 1
    tokens = micro_count * tok_mb
    mixed, expert_load = layer(
        hidden.reshape(tokens, model_width),
        expert_ids.transpose(0, 2, 1),
        gate_scores.transpose(0, 2, 1),
        w_gate[0],
        w_up[0],
        w_down[0],
        devices,
        tok_mb,
        capacity,
        devices / (route_scale * tokens * devices),
    )
    return (mixed.reshape(micro_count, tok_mb, model_width), expert_load.reshape(1))


def solution(mesh):
    placed = (
        P(None, "ep", None),
        P(None, "ep", None),
        P(None, "ep", None),
        P("ep", None, None),
        P("ep", None, None),
        P("ep", None, None),
    )
    return jax.shard_map(
        shards,
        mesh=mesh,
        in_specs=placed,
        out_specs=(P(None, "ep", None), P("ep")),
        check_vma=False,
    )
```
